256 devices in a mesh: dp: 4 (over z_hi), expert: 8 (over z_lo, x), tensor: 8 (over y, core).
Axes of the slice: x: 4, y: 4, z: 8 (z_hi: 4, z_lo: 2; z = z_hi * 2 + z_lo), core: 2. Of those that a mesh axis runs over, the one named last changes fastest.
Arguments:
- tokens: bfloat16 [2048, 4096], P(('dp', 'expert', 'tensor')), may hold values from -6 to 6
- out_grad: bfloat16 [2048, 4096], P(('dp', 'expert', 'tensor')), may hold values from -4 to 4
- route_probs: float32 [2048, 2], P(('dp', 'expert')), may hold values from 0.2 to 1
- expert_ids: int32 [2048, 2], P(('dp', 'expert')), may hold values from 0 to 7, as said below
- slot_index: int32 [2048, 2], P(('dp', 'expert')), may hold values from 0 to 20, as said below
- w_gate: bfloat16 [8, 4096, 7168], P('expert', 'dp', 'tensor'), may hold values from -0.09375 to 0.09375
- w_up: bfloat16 [8, 4096, 7168], P('expert', 'dp', 'tensor'), may hold values from -0.09375 to 0.09375
- w_down: bfloat16 [8, 7168, 4096], P('expert', 'tensor', 'dp'), may hold values from -0.0625 to 0.0625
Outputs:
- token_grad: bfloat16 [2048, 4096], P(('dp', 'expert', 'tensor'))
- grad_gate: bfloat16 [8, 4096, 7168], P('expert', 'dp', 'tensor')
- grad_up: bfloat16 [8, 4096, 7168], P('expert', 'dp', 'tensor')
- grad_down: bfloat16 [8, 7168, 4096], P('expert', 'tensor', 'dp')
The draws below stay inside these ranges and needn't reach their ends.
Inputs may be any that keep to these rules, and one draw needn't show every extreme that they name: `expert_ids`: the 2 entries of a token are different experts. slot_index[t, k] counts the earlier routes to expert_ids[t, k] within the token's routing block of 64 rows, in order of tokens and then of routes; the value 20 marks a route past the capacity, which is dropped (a count of 20 or more is given as 20). In every draw some expert is filled to 20 slots in every block.
All inputs are finite; a program needn't handle non-finite values.
Results may differ from the reference program's by a relative error of at most 0.011.
Values may be sent and summed in bfloat16 or wider, within the bound.
A program may use at most 128 MiB of HBM per device.

```python
import jax
import jax.numpy as jnp
from jax import lax

D = 4096
EXPERTS = 8
TOP = 2
FF = 7168
GROUP = 64
CAP = 20
TOKENS = 2048


def route_draw(key):
    blocks = TOKENS // GROUP
    base = jax.random.fold_in(key, 7)
    hot_key, pick_key, first_key, second_key = jax.random.split(base, 4)
    hot_expert = jax.random.randint(hot_key, (), 0, EXPERTS)
    pick = jax.random.randint(pick_key, (blocks, GROUP), 0, 2)
    first_any = jax.random.randint(first_key, (blocks, GROUP), 0, EXPERTS)
    first = jnp.where(pick == 1, hot_expert, first_any)
    second = (first + 1 + jax.random.randint(second_key, (blocks, GROUP), 0, EXPERTS - 1)) % EXPERTS
    chosen = jnp.stack([first, second], -1).astype(jnp.int32)
    flat_ids = chosen.reshape(blocks, GROUP * TOP)
    onehot = (flat_ids[:, :, None] == jnp.arange(EXPERTS, dtype=jnp.int32)[None, None, :]).astype(jnp.int32)
    earlier = jnp.cumsum(onehot, axis=1) - onehot
    position = jnp.sum(earlier * onehot, axis=-1)
    position = jnp.minimum(position, CAP).astype(jnp.int32)
    return (chosen.reshape(TOKENS, TOP), position.reshape(TOKENS, TOP))


def draw_expert_ids(key, part):
    return route_draw(key)[0]


def draw_slot_index(key, part):
    return route_draw(key)[1]


def level_of(rng, shape, cuts, low, largest):
    def one(axis_at, blocks):
        steps = jax.random.uniform(jax.random.fold_in(jax.random.fold_in(rng, 6), axis_at), (blocks,), jnp.float32, low / len(cuts), largest / len(cuts))
        return jnp.repeat(jnp.exp(steps), shape[axis_at] // blocks).reshape((-1,) + (1,) * (len(shape) - axis_at - 1))

    gain = one(*cuts[0])
    for cut in cuts[1:]:
        gain = gain * one(*cut)
    return gain


def scatter_about(own_key, extent, spread, most, cuts=(), kind=jnp.bfloat16):
    values = jax.random.normal(own_key, extent, jnp.float32) * spread
    if len(cuts) > 0:
        values = level_of(own_key, extent, cuts, -0.22, 0.18) * values
    return jnp.clip(values, min=-most, max=most).astype(kind)


def setup_inputs(seed: int = 0) -> dict:
    key_of = jax.random.split(jax.random.key(seed), 9)
    return {
        "tokens": scatter_about(key_of[0], (TOKENS, D), 1.0, 6.0, ((0, 256),)),
        "out_grad": scatter_about(key_of[1], (TOKENS, D), 0.5, 4.0, ((0, 256),)),
        "route_probs": jnp.clip(0.2 + 0.8 * jax.random.uniform(key_of[2], (TOKENS, TOP), jnp.float32) ** level_of(key_of[2], (TOKENS, TOP), ((0, 32),), -0.2, 0.2), 0.2, 1.0),
        "expert_ids": draw_expert_ids(jax.random.fold_in(key_of[8], 71), 0),
        "slot_index": draw_slot_index(jax.random.fold_in(key_of[8], 71), 0),
        "w_gate": scatter_about(key_of[5], (EXPERTS, D, FF), D ** -0.5, 0.09375, ((0, 8), (1, 4), (2, 8))),
        "w_up": scatter_about(key_of[6], (EXPERTS, D, FF), D ** -0.5, 0.09375, ((0, 8), (1, 4), (2, 8))),
        "w_down": scatter_about(key_of[7], (EXPERTS, FF, D), FF ** -0.5, 0.0625, ((0, 8), (1, 8), (2, 4))),
    }


def route_tables(expert_ids, slot_index, capacity):
    target = slot_index * EXPERTS + expert_ids
    target = jnp.where(slot_index < capacity, target, -1).astype(jnp.int32)
    places = jnp.arange(capacity * EXPERTS, dtype=jnp.int32)
    return [(places[:, None] == target[None, :, k]).astype(jnp.bfloat16) for k in range(TOP)]


def swiglu_back(pre_gate, pre_up, grad_hidden):
    sigmoid_gate = jax.nn.sigmoid(pre_gate)
    silu_gate = pre_gate * sigmoid_gate
    hidden = (silu_gate * pre_up).astype(jnp.bfloat16)
    up_delta = (grad_hidden * silu_gate).astype(jnp.bfloat16)
    gate_delta = (grad_hidden * pre_up * sigmoid_gate * (1.0 + pre_gate * (1.0 - sigmoid_gate))).astype(jnp.bfloat16)
    return hidden, gate_delta, up_delta


def reference(tokens, out_grad, route_probs, expert_ids, slot_index, w_gate, w_up, w_down):
    blocks = TOKENS // GROUP
    capacity = CAP

    def dispatch(inputs):
        block_x, block_dy, block_probs, block_ids, block_slots = inputs
        tables = route_tables(block_ids, block_slots, capacity)
        table_sum = tables[0] + tables[1]
        x_buf = jnp.dot(table_sum, block_x, preferred_element_type=jnp.float32).astype(jnp.bfloat16)
        grad_buf = jnp.zeros((capacity * EXPERTS, D), jnp.float32)
        for k in range(TOP):
            scaled = (block_probs[:, k:k + 1] * block_dy.astype(jnp.float32)).astype(jnp.bfloat16)
            grad_buf = grad_buf + jnp.dot(tables[k], scaled, preferred_element_type=jnp.float32)
        grad_buf = grad_buf.astype(jnp.bfloat16)
        return (x_buf.reshape(capacity, EXPERTS, D), grad_buf.reshape(capacity, EXPERTS, D),
                table_sum.astype(jnp.float32))

    x_bufs, grad_bufs, table_all = lax.map(dispatch, (
        tokens.reshape(blocks, GROUP, D), out_grad.reshape(blocks, GROUP, D),
        route_probs.reshape(blocks, GROUP, TOP), expert_ids.reshape(blocks, GROUP, TOP),
        slot_index.reshape(blocks, GROUP, TOP)))
    expert_x = jnp.moveaxis(x_bufs, 2, 0).reshape(EXPERTS, blocks * capacity, D)
    expert_g = jnp.moveaxis(grad_bufs, 2, 0).reshape(EXPERTS, blocks * capacity, D)

    def expert_back(inputs):
        rows_x, rows_g, gate_w, up_w, down_w = inputs
        pre_gate = jnp.dot(rows_x, gate_w, preferred_element_type=jnp.float32)
        pre_up = jnp.dot(rows_x, up_w, preferred_element_type=jnp.float32)
        grad_hidden = jnp.dot(rows_g, down_w.T, preferred_element_type=jnp.float32)
        hidden, gate_delta, up_delta = swiglu_back(pre_gate, pre_up, grad_hidden)
        g_down = jnp.dot(hidden.T, rows_g, preferred_element_type=jnp.float32).astype(jnp.bfloat16)
        g_gate = jnp.dot(rows_x.T, gate_delta, preferred_element_type=jnp.float32).astype(jnp.bfloat16)
        g_up = jnp.dot(rows_x.T, up_delta, preferred_element_type=jnp.float32).astype(jnp.bfloat16)
        row_grad = jnp.dot(gate_delta, gate_w.T, preferred_element_type=jnp.float32)
        row_grad = row_grad + jnp.dot(up_delta, up_w.T, preferred_element_type=jnp.float32)
        return g_gate, g_up, g_down, row_grad

    grad_gate, grad_up, grad_down, row_grad = lax.map(expert_back, (expert_x, expert_g, w_gate, w_up, w_down))
    row_grad = row_grad.reshape(EXPERTS, blocks, capacity, D)
    row_grad = jnp.transpose(row_grad, (1, 2, 0, 3)).reshape(blocks, capacity * EXPERTS, D)
    token_grad = jnp.einsum("bjt,bjd->btd", table_all, row_grad, precision=lax.Precision.HIGHEST)
    token_grad = token_grad.reshape(TOKENS, D).astype(jnp.bfloat16)
    return token_grad, grad_gate, grad_up, grad_down
```

```python
import functools

import jax
import jax.numpy as jnp
from jax import lax
from jax.experimental import pallas as pl
from jax.experimental.pallas import tpu as pltpu
from jax.sharding import PartitionSpec as P

BF, F32 = jnp.bfloat16, jnp.float32
MESH = pl.DeviceIdType.MESH
STAGES = 5
CAP, MAIN = 20, 16


def nt(a, b):
    return lax.dot_general(a, b, (((1,), (1,)), ((), ())), preferred_element_type=F32)


def nn(a, b):
    return jnp.dot(a, b, preferred_element_type=F32)


def remote(src, dst, send, recv, dev):
    return pltpu.make_async_remote_copy(
        src_ref=src, dst_ref=dst, send_sem=send, recv_sem=recv, device_id=dev, device_id_type=MESH
    )


def loop(n, f, start=0):
    def step(i, c):
        f(i)
        return c

    lax.fori_loop(start, n, step, 0)


def group_of(i):
    return lax.rem(2 * jnp.int32(i), jnp.int32(STAGES))


def kernel(
    sendA, tx, t0, t1, tt_ref, pp, wg_hbm, wu_hbm, wd_hbm,
    h_out, xg_out, y_out,
    wg, wu, wd, recvA, sendC, recvC, XG, part, rs1, raw, red, redS, H,
    rgp, recvP, qs, recvQ, zs, recvZ, sendY, recvY,
    wsem, sA, rA, sC, rC, sD, rD, sR, rR, sG, rG, sP, rP, sQ, rQ, sZ, rZ, sY, rY, osem,
):
    d, e, t = lax.axis_index("dp"), lax.axis_index("expert"), lax.axis_index("tensor")
    b = d * 8 + e
    core, y = lax.rem(t, 2), lax.div(t, 2)
    mate = t + 1 - 2 * core
    right, left, opp = lax.rem(d + 1, 4), lax.rem(d + 3, 4), lax.rem(d + 2, 4)

    def at_t(tt):
        return (d, e, tt)

    def at_p(p):
        return (lax.div(p, 8), lax.rem(p, 8), t)

    weights = [
        pltpu.make_async_copy(wg_hbm, wg, wsem.at[0]),
        pltpu.make_async_copy(wu_hbm, wu, wsem.at[1]),
        pltpu.make_async_copy(wd_hbm, wd, wsem.at[2]),
    ]
    for w in weights:
        w.start()

    bar = pltpu.get_barrier_semaphore()

    def greet_t(k):
        pl.semaphore_signal(bar, inc=1, device_id=at_t(lax.rem(t + k, 8)), device_id_type=MESH)

    def greet_p(k):
        pl.semaphore_signal(bar, inc=1, device_id=at_p(lax.rem(b + k, 32)), device_id_type=MESH)

    loop(32, greet_p, 1)
    loop(8, greet_t, 1)
    pl.semaphore_wait(bar, 38)

    def send_a(k):
        q = lax.rem(t + k, 8)
        return remote(sendA.at[q], recvA.at[t], sA.at[q], rA.at[t], at_t(q))

    loop(8, lambda k: send_a(k).start(), 1)
    recvA[t] = sendA[t]

    def wait_a(k):
        q = lax.rem(t + k, 8)
        remote(recvA.at[q], recvA.at[q], sA.at[q], rA.at[q], at_t(q)).wait_recv()

    loop(8, wait_a, 1)

    R = recvA[...].reshape(128, 512)
    xb = nn(tx[...], R).astype(BF)
    Rf = R.astype(F32)
    s0 = (pp[:, 0:1] * Rf).astype(BF)
    s1 = (pp[:, 1:2] * Rf).astype(BF)
    gb = (nn(t0[...], s0) + nn(t1[...], s1)).astype(BF)
    for dd in range(4):
        cols = slice(128 * dd, 128 * dd + 128)
        sendC[8 * dd : 8 * dd + 8, 0] = xb[:, cols].reshape(8, 32, 128)
        sendC[8 * dd : 8 * dd + 8, 1] = gb[:, cols].reshape(8, 32, 128)

    def send_c(k):
        p = lax.rem(b + k, 32)
        return remote(sendC.at[p], recvC.at[b], sC.at[p], rC.at[b], at_p(p))

    loop(32, lambda k: send_c(k).start(), 1)
    recvC[b] = sendC[b]

    def wait_c(p):
        @pl.when(p != b)
        def _():
            remote(recvC.at[p], recvC.at[p], sC.at[p], rC.at[p], at_p(p)).wait_recv()

    def piece(src, g):
        return XG.at[src, :, pl.ds(8 * g, 8)]

    def send_d(i, g, slot, src, dst):
        return remote(piece(src, g), piece(src, g), sD.at[i, slot], rD.at[i, src], at_t(dst))

    def wait_d(i, g, src):
        remote(piece(src, g), piece(src, g), sD.at[i, 0], rD.at[i, src], at_t(mate)).wait_recv()

    def prep_main(i):
        g = group_of(i)

        def one(j):
            p = 8 * g + j
            wait_c(p)
            XG[t, 0, p] = recvC[p, 0, 0:16]
            XG[t, 1, p] = recvC[p, 1, 0:16]

        loop(8, one)

    def start_d(i):
        g = group_of(i)
        send_d(i, g, 0, t, mate).start()
        for k in range(1, 4):
            send_d(i, g, k, t, lax.rem(t + 2 * k, 8)).start()

    def relay_d(i):
        g = group_of(i)
        for k in (1, 3, 2):
            q = lax.rem(t + 2 * k, 8)
            wait_d(i, g, q)
            send_d(i, g, 4 + k, q, mate).start()

    def arrive_d(i):
        g = group_of(i)
        for k in range(4):
            wait_d(i, g, lax.rem(mate + 2 * k, 8))

    for i in (0, 1, 3, 4):
        prep_main(i)
        start_d(i)

    def rest(j):
        for a in range(2):
            v = recvC[4 * j, a, 16:32].astype(F32)
            for q in range(1, 4):
                v = v + recvC[4 * j + q, a, 16:32].astype(F32)
            XG[t, a, 32 + j] = v.astype(BF)

    loop(8, rest)
    start_d(2)

    for w in weights:
        w.wait()

    def tile(g, owner, half):
        return 8 * g + 2 * owner + half

    def peer(dd):
        return (dd, e, t)

    def rs_send(i, m):
        g = group_of(i)
        src, dst, dev = {
            0: (part.at[:, tile(g, opp, 0)], rs1.at[0, i], right),
            1: (part.at[:, tile(g, right, 1)], raw.at[0, i], right),
            2: (redS.at[0, i], red.at[0, i], right),
            3: (part.at[:, tile(g, opp, 1)], rs1.at[1, i], left),
            4: (part.at[:, tile(g, left, 0)], raw.at[1, i], left),
            5: (redS.at[1, i], red.at[1, i], left),
        }[m]
        return remote(src, dst, sR.at[i, m], rR.at[i, m], peer(dev))

    def rs_wait(i, m):
        dst = (rs1, raw, red)[m % 3].at[m // 3, i]
        remote(dst, dst, sR.at[i, m], rR.at[i, m], peer(right)).wait_recv()

    def forward(i):
        @pl.when(i < STAGES - 1)
        def _():
            relay_d(i + 1)

        arrive_d(i)
        g = group_of(i)
        tiles = pl.ds(8 * g, 8)
        xs = jnp.concatenate([XG[q, 0, tiles].reshape(128, 128) for q in range(8)], axis=1)
        part[0, tiles] = nn(xs, wg[...]).astype(BF).reshape(8, 16, -1)
        part[1, tiles] = nn(xs, wu[...]).astype(BF).reshape(8, 16, -1)
        gs = jnp.concatenate([XG[q, 1, tiles].reshape(128, 128) for q in range(8)], axis=1)
        part[2, tiles] = nt(gs, wd[...]).astype(BF).reshape(8, 16, -1)
        for m in (0, 3, 1, 4):
            rs_send(i, m).start()

    relay_d(0)
    loop(STAGES, forward)

    outs = [
        pltpu.make_async_copy(XG.at[q], xg_out.at[:, :, :, pl.ds(128 * q, 128)], osem.at[q])
        for q in range(8)
    ]
    for o in outs:
        o.start()

    def middle(i):
        g = group_of(i)
        rs_wait(i, 0)
        redS[0, i] = (part[:, tile(g, right, 0)].astype(F32) + rs1[0, i].astype(F32)).astype(BF)
        rs_send(i, 2).start()
        rs_wait(i, 3)
        redS[1, i] = (part[:, tile(g, left, 1)].astype(F32) + rs1[1, i].astype(F32)).astype(BF)
        rs_send(i, 5).start()

    loop(STAGES, middle)

    def ag_send(i, m):
        g = group_of(i)
        src, dev = {
            0: (H.at[:, pl.ds(tile(g, d, 0), 2)], right),
            1: (H.at[:, pl.ds(tile(g, d, 0), 2)], left),
            2: (H.at[:, tile(g, left, 0)], right),
            3: (H.at[:, tile(g, right, 1)], left),
        }[m]
        return remote(src, src, sG.at[i, m], rG.at[i, m], peer(dev))

    def ag_wait(i, m):
        g = group_of(i)
        dst = (
            H.at[:, pl.ds(tile(g, left, 0), 2)],
            H.at[:, pl.ds(tile(g, right, 0), 2)],
            H.at[:, tile(g, opp, 0)],
            H.at[:, tile(g, opp, 1)],
        )[m]
        remote(dst, dst, sG.at[i, m], rG.at[i, m], peer(right)).wait_recv()

    def own(i):
        g = group_of(i)
        rs_wait(i, 1)
        rs_wait(i, 4)
        for half, (ra, rb, m) in enumerate(((red, raw, 2), (raw, red, 5))):
            rs_wait(i, m)
            at = tile(g, d, half)
            pre = [
                part[u, at].astype(F32) + ra[0, i, u].astype(F32) + rb[1, i, u].astype(F32)
                for u in range(3)
            ]
            gate, up, grad = pre
            s = jax.nn.sigmoid(gate)
            silu = gate * s
            H[0, at] = (silu * up).astype(BF)
            H[1, at] = (grad * up * s * (1.0 + gate * (1.0 - s))).astype(BF)
            H[2, at] = (grad * silu).astype(BF)
        ag_send(i, 0).start()
        ag_send(i, 1).start()

    loop(STAGES, own)

    def relay(i):
        ag_wait(i, 0)
        ag_send(i, 2).start()
        ag_wait(i, 1)
        ag_send(i, 3).start()

    loop(STAGES, relay)

    def p_copy(i):
        return remote(rgp.at[i, 1 - core], recvP.at[i], sP.at[i], rP.at[i], at_t(mate))

    def q_send(i, k):
        yy = lax.rem(y + k, 4)
        return remote(qs.at[i, yy], recvQ.at[i, y], sQ.at[i, yy], rQ.at[i, y], at_t(2 * yy + core))

    def rows(i):
        ag_wait(i, 2)
        ag_wait(i, 3)
        g = group_of(i)
        tiles = pl.ds(8 * g, 8)
        rg = nt(H[1, tiles].reshape(128, -1), wg[...]) + nt(H[2, tiles].reshape(128, -1), wu[...])
        for q in range(8):
            rgp[i, q % 2, q // 2] = rg[:, 128 * q : 128 * q + 128].astype(BF)
        p_copy(i).start()

    def pair(i):
        remote(recvP.at[i], recvP.at[i], sP.at[i], rP.at[i], at_t(mate)).wait_recv()
        qs[i] = (rgp[i, core].astype(F32) + recvP[i].astype(F32)).astype(BF)
        for k in (2, 1, 3):
            q_send(i, k).start()

    def z_main(i, j):
        p = 8 * group_of(i) + j
        return p, remote(zs.at[i, j], recvZ.at[b, 0], sZ.at[0, p], rZ.at[0, b], at_p(p))

    def z_rest(p):
        return remote(zs.at[2, lax.div(p, 4)], recvZ.at[b, 1], sZ.at[1, p], rZ.at[1, b], at_p(p))

    def back(i):
        tot = qs[i, y].astype(F32)
        for k in range(1, 4):
            yy = lax.rem(y + k, 4)
            remote(recvQ.at[i, yy], recvQ.at[i, yy], sQ.at[i, yy], rQ.at[i, yy], at_t(mate)).wait_recv()
            tot = tot + recvQ[i, yy].astype(F32)
        zs[i] = tot.astype(BF).reshape(8, 16, 128)

        @pl.when(group_of(i) < 4)
        def _():
            def one(j):
                p, copy = z_main(i, j)

                @pl.when(p != b)
                def _():
                    copy.start()

                @pl.when(p == b)
                def _():
                    recvZ[b, 0] = zs[i, j]

            loop(8, one)

        @pl.when(group_of(i) == 4)
        def _():
            loop(32, lambda k: z_rest(lax.rem(b + k, 32)).start(), 1)
            recvZ[b, 1] = zs[2, lax.div(b, 4)]

    def finish(i):
        rows(i)

        @pl.when(i >= 1)
        def _():
            pair(i - 1)

        @pl.when(i >= 2)
        def _():
            back(i - 2)

    loop(STAGES, finish)
    houts = [pltpu.make_async_copy(H, h_out, osem.at[8])]
    for o in houts:
        o.start()
    pair(STAGES - 1)
    back(STAGES - 2)
    back(STAGES - 1)

    def wait_z(k):
        p = lax.rem(b + k, 32)
        for w in range(2):
            remote(recvZ.at[p, w], recvZ.at[p, w], sZ.at[w, p], rZ.at[w, p], at_p(p)).wait_recv()

    loop(32, wait_z, 1)
    for dd in range(4):
        z = recvZ[8 * dd : 8 * dd + 8].reshape(256, 128)
        sendY[:, :, 128 * dd : 128 * dd + 128] = nn(tt_ref[...], z).astype(BF).reshape(8, 16, 128)

    def y_copy(k):
        q = lax.rem(t + k, 8)
        return remote(sendY.at[q], recvY.at[t], sY.at[q], rY.at[t], at_t(q))

    loop(8, lambda k: y_copy(k).start(), 1)
    recvY[t] = sendY[t]

    def wait_y(k):
        q = lax.rem(t + k, 8)
        remote(recvY.at[q], recvY.at[q], sY.at[q], rY.at[q], at_t(q)).wait_recv()

    loop(8, wait_y, 1)
    y_out[...] = recvY[...]

    loop(8, lambda k: send_a(k).wait_send(), 1)
    loop(32, lambda k: send_c(k).wait_send(), 1)

    def drain(i):
        g = group_of(i)
        send_d(i, g, 0, t, mate).wait_send()
        for k in range(1, 4):
            send_d(i, g, k, t, mate).wait_send()
            send_d(i, g, 4 + k, t, mate).wait_send()
        for m in range(6):
            rs_send(i, m).wait_send()
        for m in range(4):
            ag_send(i, m).wait_send()
        p_copy(i).wait_send()
        for k in range(1, 4):
            q_send(i, k).wait_send()

        @pl.when(g < 4)
        def _():
            def one(j):
                p, copy = z_main(i, j)

                @pl.when(p != b)
                def _():
                    copy.wait_send()

            loop(8, one)

    loop(STAGES, drain)
    loop(32, lambda k: z_rest(lax.rem(b + k, 32)).wait_send(), 1)
    loop(8, lambda k: y_copy(k).wait_send(), 1)
    for o in outs + houts:
        o.wait()


def tables(route_probs, expert_ids, slot_index):
    e = lax.axis_index("expert")
    row = jnp.where(slot_index < MAIN, slot_index, slot_index + 4 * lax.rem(e, 4))
    place = jnp.where(slot_index < CAP, expert_ids * 32 + row, -1)
    place = place.T.reshape(2, 8, 8)
    none = jnp.full_like(place, -1)
    at_x = jnp.concatenate([place, none], axis=2).reshape(2, 128)
    at_g = jnp.concatenate([none, place], axis=2).reshape(2, 128)
    places = jnp.arange(256, dtype=jnp.int32)
    tx = ((places[:, None] == at_x[0]) | (places[:, None] == at_x[1])).astype(BF)
    tt = ((places == at_x[0][:, None]) | (places == at_x[1][:, None])).astype(BF)
    t0 = (places[:, None] == at_g[0]).astype(BF)
    t1 = (places[:, None] == at_g[1]).astype(BF)
    probs = route_probs.reshape(8, 8, 2)
    probs = jnp.concatenate([jnp.zeros_like(probs), probs], axis=1).reshape(128, 2)
    return tx, t0, t1, tt, probs


def shards(tokens, out_grad, route_probs, expert_ids, slot_index, w_gate, w_up, w_down):
    tx, t0, t1, tt, probs = tables(route_probs, expert_ids, slot_index)
    both = jnp.stack([tokens, out_grad], 0).reshape(2, 8, 4, 8, 128)
    both = jnp.transpose(both, (3, 0, 1, 2, 4)).reshape(8, 16, 512)
    wg, wu, wd = w_gate[0], w_up[0], w_down[0]
    dl, fl = wg.shape
    vm = pl.BlockSpec(memory_space=pltpu.VMEM)
    hbm = pl.BlockSpec(memory_space=pl.ANY)
    S = STAGES
    dma = pltpu.SemaphoreType.DMA
    h, xg, yv = pl.pallas_call(
        kernel,
        name="expert_back",
        out_shape=(
            jax.ShapeDtypeStruct((3, 40, 16, fl), BF),
            jax.ShapeDtypeStruct((2, 40, 16, dl), BF),
            jax.ShapeDtypeStruct((8, 16, 512), BF),
        ),
        in_specs=[vm] * 6 + [hbm] * 3,
        out_specs=(hbm, hbm, vm),
        scratch_shapes=[
            pltpu.VMEM((dl, fl), BF),
            pltpu.VMEM((dl, fl), BF),
            pltpu.VMEM((fl, dl), BF),
            pltpu.VMEM((8, 16, 512), BF),
            pltpu.VMEM((32, 2, 32, 128), BF),
            pltpu.VMEM((32, 2, 32, 128), BF),
            pltpu.VMEM((8, 2, 40, 16, 128), BF),
            pltpu.VMEM((3, 40, 16, fl), BF),
            pltpu.VMEM((2, S, 3, 16, fl), BF),
            pltpu.VMEM((2, S, 3, 16, fl), BF),
            pltpu.VMEM((2, S, 3, 16, fl), BF),
            pltpu.VMEM((2, S, 3, 16, fl), BF),
            pltpu.VMEM((3, 40, 16, fl), BF),
            pltpu.VMEM((S, 2, 4, 128, 128), BF),
            pltpu.VMEM((S, 4, 128, 128), BF),
            pltpu.VMEM((S, 4, 128, 128), BF),
            pltpu.VMEM((S, 4, 128, 128), BF),
            pltpu.VMEM((S, 8, 16, 128), BF),
            pltpu.VMEM((32, 2, 16, 128), BF),
            pltpu.VMEM((8, 16, 512), BF),
            pltpu.VMEM((8, 16, 512), BF),
            dma((3,)), dma((8,)), dma((8,)), dma((32,)), dma((32,)),
            dma((S, 8)), dma((S, 8)), dma((S, 6)), dma((S, 6)), dma((S, 4)), dma((S, 4)),
            dma((S,)), dma((S,)), dma((S, 4)), dma((S, 4)), dma((2, 32)), dma((2, 32)),
            dma((8,)), dma((8,)), dma((9,)),
        ],
        compiler_params=pltpu.CompilerParams(
            collective_id=0, has_side_effects=True, vmem_limit_bytes=60 * 1024 * 1024
        ),
    )(both, tx, t0, t1, tt, probs, wg, wu, wd)
    h = h.reshape(3, 640, fl)
    xg = xg.reshape(2, 640, dl)

    def tn(a, c):
        return lax.dot_general(a, c, (((0,), (0,)), ((), ())), preferred_element_type=F32).astype(BF)[None]

    grad_down = tn(h[0], xg[1])
    grad_gate = tn(xg[0], h[1])
    grad_up = tn(xg[0], h[2])
    token_grad = yv[:, :8].reshape(8, 8, 4, 128)
    token_grad = jnp.transpose(token_grad, (1, 2, 0, 3)).reshape(8, 4096)
    return token_grad, grad_gate, grad_up, grad_down


def solution(mesh):
    placed = (
        P(("dp", "expert", "tensor"), None),
        P(("dp", "expert", "tensor"), None),
        P(("dp", "expert"), None),
        P(("dp", "expert"), None),
        P(("dp", "expert"), None),
        P("expert", "dp", "tensor"),
        P("expert", "dp", "tensor"),
        P("expert", "tensor", "dp"),
    )
    return jax.shard_map(
        shards,
        mesh=mesh,
        in_specs=placed,
        out_specs=(
            P(("dp", "expert", "tensor"), None),
            P("expert", "dp", "tensor"),
            P("expert", "dp", "tensor"),
            P("expert", "tensor", "dp"),
        ),
        check_vma=False,
    )
```

```python
import jax
import jax.numpy as jnp
from jax import lax
from jax.experimental import pallas as pl
from jax.experimental.pallas import tpu as pltpu
from jax.sharding import PartitionSpec as P

BF, F32 = jnp.bfloat16, jnp.float32
MESH = pl.DeviceIdType.MESH
S = 5
CAP = 20
PLACES = 192


def nt(a, b):
    return lax.dot_general(a, b, (((1,), (1,)), ((), ())), preferred_element_type=F32)


def tn(a, b):
    return lax.dot_general(a, b, (((0,), (0,)), ((), ())), preferred_element_type=F32)


def nn(a, b):
    return jnp.dot(a, b, preferred_element_type=F32)


def remote(src, dst, send, recv, dev):
    return pltpu.make_async_remote_copy(
        src_ref=src, dst_ref=dst, send_sem=send, recv_sem=recv, device_id=dev, device_id_type=MESH
    )


def loop(n, f, start=0):
    def step(i, c):
        f(i)
        return c

    lax.fori_loop(start, n, step, 0)


def column(row):
    n = row.shape[1]
    eye = lax.broadcasted_iota(jnp.int32, (n, n), 0) == lax.broadcasted_iota(jnp.int32, (n, n), 1)
    spread = jnp.where(eye, jnp.broadcast_to(row, (n, n)), jnp.zeros((n, n), row.dtype))
    return jnp.sum(spread, axis=1, keepdims=True)


def kernel(
    tok_hbm, og_hbm, prob_hbm, id_hbm, slot_hbm, wg_hbm, wu_hbm, wd_hbm,
    y_out, gg_out, gu_out, gd_out,
    tok, og, prob, ids, slots, wg, wu, wd, tab,
    sendA, recvA, sendC, recvC, XG, XT, part, rs1, raw, red, redS, H,
    rgp, recvP, qs, recvQ, zs, recvZ, sendY, recvY, accg, accd, outg, outd,
    isem, wsem, sA, rA, sC, rC, sD, rD, sR, rR, sG, rG, sP, rP, sQ, rQ, sZ, rZ, sY, rY, osem,
):
    d, e, t = lax.axis_index("dp"), lax.axis_index("expert"), lax.axis_index("tensor")
    b = d * 8 + e
    core, y = lax.rem(t, 2), lax.div(t, 2)
    mate = t + 1 - 2 * core
    right, left, opp = lax.rem(d + 1, 4), lax.rem(d + 3, 4), lax.rem(d + 2, 4)

    def at_t(tt):
        return (d, e, tt)

    def at_p(p):
        return (lax.div(p, 8), lax.rem(p, 8), t)

    bar = pltpu.get_barrier_semaphore()

    def greet_t(k):
        pl.semaphore_signal(bar, inc=1, device_id=at_t(lax.rem(t + k, 8)), device_id_type=MESH)

    def greet_p(k):
        pl.semaphore_signal(bar, inc=1, device_id=at_p(lax.rem(b + k, 32)), device_id_type=MESH)

    loop(32, greet_p, 1)
    loop(8, greet_t, 1)

    inputs = [
        pltpu.make_async_copy(src, dst, isem.at[n])
        for n, (src, dst) in enumerate(
            ((tok_hbm, tok), (og_hbm, og), (prob_hbm, prob), (id_hbm, ids), (slot_hbm, slots))
        )
    ]
    weights = [
        pltpu.make_async_copy(src, dst, wsem.at[n])
        for n, (src, dst) in enumerate(((wg_hbm, wg), (wu_hbm, wu), (wd_hbm, wd)))
    ]
    for c in inputs + weights:
        c.start()
    for c in inputs:
        c.wait()
    for dd in range(4):
        for q in range(8):
            at = slice(1024 * dd + 128 * q, 1024 * dd + 128 * q + 128)
            sendA[q, 0, :, 128 * dd : 128 * dd + 128] = tok[:, at]
            sendA[q, 1, :, 128 * dd : 128 * dd + 128] = og[:, at]
    slot, owner = slots[...], ids[...] * 8
    place = jnp.where(
        slot >= 16,
        owner + 4 * lax.rem(e, 2) + slot - 16,
        jnp.where(slot < 8, 64 + owner + slot, 120 + owner + slot),
    )
    place = jnp.where(slot < CAP, place, -1)
    by_place = lax.broadcasted_iota(jnp.int32, (PLACES, 64), 0)
    t0, t1 = ((by_place == place[k : k + 1]).astype(F32) for k in range(2))
    tx, t0, t1 = (t0 + t1).astype(BF), t0.astype(BF), t1.astype(BF)
    by_token = lax.broadcasted_iota(jnp.int32, (64, PLACES), 1)
    tab[...] = sum((by_token == column(place[k : k + 1])).astype(F32) for k in range(2)).astype(BF)
    p0, p1 = (column(prob[k : k + 1]) for k in range(2))
    pl.semaphore_wait(bar, 38)

    def send_a(k):
        q = lax.rem(t + k, 8)
        return remote(sendA.at[q], recvA.at[t], sA.at[q], rA.at[t], at_t(q))

    loop(8, lambda k: send_a(k).start(), 1)
    recvA[t] = sendA[t]

    def wait_a(k):
        q = lax.rem(t + k, 8)
        remote(recvA.at[q], recvA.at[q], sA.at[q], rA.at[q], at_t(q)).wait_recv()

    loop(8, wait_a, 1)

    rx = recvA[:, 0].astype(F32).reshape(64, 512).astype(BF)
    ry = recvA[:, 1].astype(F32).reshape(64, 512)
    xb = nn(tx, rx)
    gb = nn(t0, (p0 * ry).astype(BF)) + nn(t1, (p1 * ry).astype(BF))
    for c in range(3):
        for dd in range(4):
            cut = slice(64 * c, 64 * c + 64), slice(128 * dd, 128 * dd + 128)
            for a, v in enumerate((xb, gb)):
                sendC[c, 8 * dd : 8 * dd + 8, a] = v[cut].reshape(8, 8, 128).astype(BF)

    def send_c(c, k):
        p = lax.rem(b + k, 32)
        return remote(sendC.at[c, p], recvC.at[c, b], sC.at[c, p], rC.at[c, b], at_p(p))

    for c in range(3):
        loop(32, lambda k, c=c: send_c(c, k).start(), 1)
        recvC[c, b] = sendC[c, b]

    def wait_c(c, p):
        @pl.when(p != b)
        def _():
            ref = recvC.at[c, p]
            remote(ref, ref, sC.at[c, p], rC.at[c, p], at_p(p)).wait_recv()

    def piece(src, i):
        return XG.at[src, :, pl.ds(8 * i, 8)]

    def send_d(i, slot, src, dst):
        return remote(piece(src, i), piece(src, i), sD.at[i, slot], rD.at[i, src], at_t(dst))

    def wait_d(i, src):
        remote(piece(src, i), piece(src, i), sD.at[i, 0], rD.at[i, src], at_t(mate)).wait_recv()

    def octet(c, p, a):
        return recvC[c, p, a].astype(F32)

    def start_d(i):
        send_d(i, 0, t, mate).start()
        for k in range(1, 4):
            send_d(i, k, t, lax.rem(t + 2 * k, 8)).start()

    def relay_d(i):
        for k in (1, 3, 2):
            q = lax.rem(t + 2 * k, 8)
            wait_d(i, q)
            send_d(i, 4 + k, q, mate).start()

    def arrive_d(i):
        for k in range(4):
            wait_d(i, lax.rem(mate + 2 * k, 8))

    loop(32, lambda p: wait_c(0, p))

    def rest(j):
        for a in range(2):
            lo = octet(0, 4 * j, a) + octet(0, 4 * j + 1, a)
            hi = octet(0, 4 * j + 2, a) + octet(0, 4 * j + 3, a)
            XG[t, a, j] = jnp.concatenate([lo, hi], axis=0).astype(BF)

    loop(8, rest)
    start_d(0)

    def prep(i):
        c, first = lax.div(i + 1, 2), 16 * lax.rem(i + 1, 2)

        def one(j):
            p = first + 2 * j
            wait_c(c, p)
            wait_c(c, p + 1)
            for a in range(2):
                both = jnp.concatenate([octet(c, p, a), octet(c, p + 1, a)], axis=0)
                XG[t, a, 8 * i + j] = both.astype(BF)

        loop(8, one)
        start_d(i)

    def tile(i, owner, half):
        return 8 * i + 2 * owner + half

    def peer(dd):
        return (dd, e, t)

    def rs_send(i, m):
        src, dst, dev = {
            0: (part.at[:, tile(i, opp, 0)], rs1.at[0, i], right),
            1: (part.at[:, tile(i, right, 1)], raw.at[0, i], right),
            2: (redS.at[0, i], red.at[0, i], right),
            3: (part.at[:, tile(i, opp, 1)], rs1.at[1, i], left),
            4: (part.at[:, tile(i, left, 0)], raw.at[1, i], left),
            5: (redS.at[1, i], red.at[1, i], left),
        }[m]
        return remote(src, dst, sR.at[i, m], rR.at[i, m], peer(dev))

    def rs_wait(i, m):
        dst = (rs1, raw, red)[m % 3].at[m // 3, i]
        remote(dst, dst, sR.at[i, m], rR.at[i, m], peer(right)).wait_recv()

    def rows_of(a, i):
        tiles = pl.ds(8 * i, 8)
        return jnp.concatenate([XG[q, a, tiles].reshape(128, 128) for q in range(8)], axis=1)

    def forward(i):
        tiles = pl.ds(8 * i, 8)
        xs = rows_of(0, i)
        part[0, tiles] = nn(xs, wg[...]).astype(BF).reshape(8, 16, -1)
        part[1, tiles] = nn(xs, wu[...]).astype(BF).reshape(8, 16, -1)
        part[2, tiles] = nt(rows_of(1, i), wd[...]).astype(BF).reshape(8, 16, -1)
        for m in (0, 3, 1, 4):
            rs_send(i, m).start()

    for c in weights:
        c.wait()

    def open_stage(i):
        @pl.when(i < S - 1)
        def _():
            prep(i + 1)

        relay_d(i)
        arrive_d(i)
        forward(i)

    loop(S, open_stage)

    def middle(i):
        rs_wait(i, 0)
        redS[0, i] = (part[:, tile(i, right, 0)].astype(F32) + rs1[0, i].astype(F32)).astype(BF)
        rs_send(i, 2).start()
        rs_wait(i, 3)
        redS[1, i] = (part[:, tile(i, left, 1)].astype(F32) + rs1[1, i].astype(F32)).astype(BF)
        rs_send(i, 5).start()

    loop(S, middle)

    def ag_send(i, m):
        src, dev = {
            0: (H.at[:, pl.ds(tile(i, d, 0), 2)], right),
            1: (H.at[:, pl.ds(tile(i, d, 0), 2)], left),
            2: (H.at[:, tile(i, left, 0)], right),
            3: (H.at[:, tile(i, right, 1)], left),
        }[m]
        return remote(src, src, sG.at[i, m], rG.at[i, m], peer(dev))

    def ag_wait(i, m):
        dst = (
            H.at[:, pl.ds(tile(i, left, 0), 2)],
            H.at[:, pl.ds(tile(i, right, 0), 2)],
            H.at[:, tile(i, opp, 0)],
            H.at[:, tile(i, opp, 1)],
        )[m]
        remote(dst, dst, sG.at[i, m], rG.at[i, m], peer(right)).wait_recv()

    def own(i):
        rs_wait(i, 1)
        rs_wait(i, 4)
        for half, (ra, rb, m) in enumerate(((red, raw, 2), (raw, red, 5))):
            rs_wait(i, m)
            at = tile(i, d, half)
            gate, up, grad = (
                part[u, at].astype(F32) + ra[0, i, u].astype(F32) + rb[1, i, u].astype(F32)
                for u in range(3)
            )
            s = jax.nn.sigmoid(gate)
            silu = gate * s
            H[0, at] = (silu * up).astype(BF)
            H[1, at] = (grad * up * s * (1.0 + gate * (1.0 - s))).astype(BF)
            H[2, at] = (grad * silu).astype(BF)
        ag_send(i, 0).start()
        ag_send(i, 1).start()

    def relay(i):
        ag_wait(i, 0)
        ag_send(i, 2).start()
        ag_wait(i, 1)
        ag_send(i, 3).start()

    def p_copy(i):
        return remote(rgp.at[i, 1 - core], recvP.at[i], sP.at[i], rP.at[i], at_t(mate))

    def q_send(i, k):
        yy = lax.rem(y + k, 4)
        return remote(qs.at[i, yy], recvQ.at[i, y], sQ.at[i, yy], rQ.at[i, y], at_t(2 * yy + core))

    def hid(u, i):
        return H[u, pl.ds(8 * i, 8)].reshape(128, -1)

    def rows(i):
        ag_wait(i, 2)
        ag_wait(i, 3)
        rg = nt(hid(1, i), wg[...]) + nt(hid(2, i), wu[...])
        for q in range(8):
            rgp[i, q % 2, q // 2] = rg[:, 128 * q : 128 * q + 128].astype(BF)
        p_copy(i).start()

    def pair(i):
        remote(recvP.at[i], recvP.at[i], sP.at[i], rP.at[i], at_t(mate)).wait_recv()
        qs[i] = (rgp[i, core].astype(F32) + recvP[i].astype(F32)).astype(BF)
        for k in (2, 1, 3):
            q_send(i, k).start()

    def z_main(i, o):
        c, p = lax.div(i + 1, 2), 16 * lax.rem(i + 1, 2) + o
        return c, p, remote(zs.at[i, o], recvZ.at[c, b], sZ.at[c, p], rZ.at[c, b], at_p(p))

    def z_rest(p):
        return remote(zs.at[0, lax.div(p, 2)], recvZ.at[0, b], sZ.at[0, p], rZ.at[0, b], at_p(p))

    def back(i):
        tot = qs[i, y].astype(F32)
        for k in (1, 3, 2):
            yy = lax.rem(y + k, 4)
            remote(recvQ.at[i, yy], recvQ.at[i, yy], sQ.at[i, yy], rQ.at[i, yy], at_t(mate)).wait_recv()
            tot = tot + recvQ[i, yy].astype(F32)
        zs[i] = tot.reshape(16, 8, 128).astype(BF)

        @pl.when(i > 0)
        def _():
            def one(o):
                c, p, copy = z_main(i, o)

                @pl.when(p != b)
                def _():
                    copy.start()

                @pl.when(p == b)
                def _():
                    recvZ[c, b] = zs[i, o]

            loop(16, one)

        @pl.when(i == 0)
        def _():
            loop(32, lambda k: z_rest(lax.rem(b + k, 32)).start(), 1)
            recvZ[0, b] = zs[0, lax.div(b, 2)]

    def turn(i):
        for q in range(8):
            v = XG[q, 0, pl.ds(8 * i, 8)].reshape(128, 128)
            XT[128 * q : 128 * q + 128, pl.ds(pl.multiple_of(128 * i, 128), 128)] = v.T

    def early_grads():
        n = 24
        for u in (1, 2):
            accg[u - 1] = nn(XT[:, : 16 * n], H[u, :n].reshape(16 * n, -1))
        g = jnp.concatenate([XG[q, 1, :n].reshape(16 * n, 128) for q in range(8)], axis=1)
        accd[...] = tn(H[0, :n].reshape(16 * n, -1), g)

    def late_grads(u):
        n = 24
        hv = H[u, n:].reshape(640 - 16 * n, -1)
        if u:
            outg[u - 1] = (accg[u - 1] + nn(XT[:, 16 * n :], hv)).astype(BF)
        else:
            g = jnp.concatenate([XG[q, 1, n:].reshape(640 - 16 * n, 128) for q in range(8)], axis=1)
            outd[...] = (accd[...] + tn(hv, g)).astype(BF)
        grads_out[u].start()

    grads_out = [
        pltpu.make_async_copy(outd, gd_out.at[0], osem.at[0]),
        pltpu.make_async_copy(outg.at[0], gg_out.at[0], osem.at[1]),
        pltpu.make_async_copy(outg.at[1], gu_out.at[0], osem.at[2]),
    ]

    loop(S, turn)
    own(0)
    own(1)
    relay(0)

    def cycle(i):
        @pl.when(i + 2 < S)
        def _():
            own(i + 2)

        @pl.when(i + 1 < S)
        def _():
            relay(i + 1)

        @pl.when(i >= 1)
        def _():
            pair(i - 1)

        @pl.when(i >= 2)
        def _():
            back(i - 2)

        rows(i)

    loop(3, cycle)
    early_grads()
    loop(S, cycle, 3)
    late_grads(1)
    pair(S - 1)
    back(S - 2)
    late_grads(2)
    back(S - 1)
    late_grads(0)

    def wait_z(k):
        p = lax.rem(b + k, 32)
        for c in range(3):
            ref = recvZ.at[c, p]
            remote(ref, ref, sZ.at[c, p], rZ.at[c, p], at_p(p)).wait_recv()

    loop(32, wait_z, 1)
    for dd in range(4):
        z = recvZ[:, 8 * dd : 8 * dd + 8].astype(F32).reshape(PLACES, 128).astype(BF)
        part_rows = nn(tab[...], z).reshape(8, 8, 128).astype(BF)
        sendY[:, :, 128 * dd : 128 * dd + 128] = part_rows

    def y_copy(k):
        q = lax.rem(t + k, 8)
        return remote(sendY.at[q], recvY.at[t], sY.at[q], rY.at[t], at_t(q))

    loop(8, lambda k: y_copy(k).start(), 1)
    recvY[t] = sendY[t]

    loop(8, lambda k: send_a(k).wait_send(), 1)
    for c in range(3):
        loop(32, lambda k, c=c: send_c(c, k).wait_send(), 1)

    def drain(i):
        for k in range(4):
            send_d(i, k, t, mate).wait_send()
        for k in range(1, 4):
            send_d(i, 4 + k, t, mate).wait_send()
            q_send(i, k).wait_send()
        for m in range(6):
            rs_send(i, m).wait_send()
        for m in range(4):
            ag_send(i, m).wait_send()
        p_copy(i).wait_send()

        @pl.when(i > 0)
        def _():
            def one(o):
                c, p, copy = z_main(i, o)

                @pl.when(p != b)
                def _():
                    copy.wait_send()

            loop(16, one)

    loop(S, drain)
    loop(32, lambda k: z_rest(lax.rem(b + k, 32)).wait_send(), 1)

    def wait_y(k):
        q = lax.rem(t + k, 8)
        remote(recvY.at[q], recvY.at[q], sY.at[q], rY.at[q], at_t(q)).wait_recv()

    loop(8, wait_y, 1)
    for dd in range(4):
        for q in range(8):
            at = slice(1024 * dd + 128 * q, 1024 * dd + 128 * q + 128)
            y_out[:, at] = recvY[q, :, 128 * dd : 128 * dd + 128]
    loop(8, lambda k: y_copy(k).wait_send(), 1)
    for c in grads_out:
        c.wait()


def shards(tokens, out_grad, route_probs, expert_ids, slot_index, w_gate, w_up, w_down):
    wg, wu, wd = w_gate[0], w_up[0], w_down[0]
    dl, fl = wg.shape
    vm = pl.BlockSpec(memory_space=pltpu.VMEM)
    hbm = pl.BlockSpec(memory_space=pl.ANY)
    dma = pltpu.SemaphoreType.DMA

    def buf(*shape, dtype=BF):
        return pltpu.VMEM(shape, dtype)

    yv, gg, gu, gd = pl.pallas_call(
        kernel,
        name="expert_back",
        out_shape=(
            jax.ShapeDtypeStruct(tokens.shape, BF),
            jax.ShapeDtypeStruct(w_gate.shape, BF),
            jax.ShapeDtypeStruct(w_up.shape, BF),
            jax.ShapeDtypeStruct(w_down.shape, BF),
        ),
        in_specs=[hbm] * 8,
        out_specs=(vm, hbm, hbm, hbm),
        scratch_shapes=[
            buf(8, 4096), buf(8, 4096), buf(2, 64, dtype=F32),
            buf(2, 64, dtype=jnp.int32), buf(2, 64, dtype=jnp.int32),
            buf(dl, fl), buf(dl, fl), buf(fl, dl), buf(64, PLACES),
            buf(8, 2, 8, 512), buf(8, 2, 8, 512),
            buf(3, 32, 2, 8, 128), buf(3, 32, 2, 8, 128),
            buf(8, 2, 40, 16, 128), buf(dl, 640), buf(3, 40, 16, fl),
            buf(2, S, 3, 16, fl), buf(2, S, 3, 16, fl), buf(2, S, 3, 16, fl), buf(2, S, 3, 16, fl),
            buf(3, 40, 16, fl),
            buf(S, 2, 4, 128, 128), buf(S, 4, 128, 128), buf(S, 4, 128, 128), buf(S, 4, 128, 128),
            buf(S, 16, 8, 128), buf(3, 32, 8, 128), buf(8, 8, 512), buf(8, 8, 512),
            buf(2, dl, fl, dtype=F32), buf(fl, dl, dtype=F32), buf(2, dl, fl), buf(fl, dl),
            dma((5,)), dma((3,)), dma((8,)), dma((8,)), dma((3, 32)), dma((3, 32)),
            dma((S, 8)), dma((S, 8)), dma((S, 6)), dma((S, 6)), dma((S, 4)), dma((S, 4)),
            dma((S,)), dma((S,)), dma((S, 4)), dma((S, 4)), dma((3, 32)), dma((3, 32)),
            dma((8,)), dma((8,)), dma((3,)),
        ],
        compiler_params=pltpu.CompilerParams(
            collective_id=0, has_side_effects=True, vmem_limit_bytes=60 * 1024 * 1024
        ),
    )(tokens, out_grad, route_probs.T, expert_ids.T, slot_index.T, wg, wu, wd)
    return yv, gg, gu, gd


def solution(mesh):
    placed = (
        P(("dp", "expert", "tensor"), None),
        P(("dp", "expert", "tensor"), None),
        P(("dp", "expert"), None),
        P(("dp", "expert"), None),
        P(("dp", "expert"), None),
        P("expert", "dp", "tensor"),
        P("expert", "dp", "tensor"),
        P("expert", "tensor", "dp"),
    )
    return jax.shard_map(
        shards,
        mesh=mesh,
        in_specs=placed,
        out_specs=(
            P(("dp", "expert", "tensor"), None),
            P("expert", "dp", "tensor"),
            P("expert", "dp", "tensor"),
            P("expert", "tensor", "dp"),
        ),
        check_vma=False,
    )
```

```python
import jax
import jax.numpy as jnp
from jax import lax
from jax.experimental import pallas as pl
from jax.experimental.pallas import tpu as pltpu
from jax.sharding import PartitionSpec as P

BF, F32 = jnp.bfloat16, jnp.float32
MESH = pl.DeviceIdType.MESH
S = 5
CAP = 20
PLACES = 192


def nt(a, b):
    return lax.dot_general(a, b, (((1,), (1,)), ((), ())), preferred_element_type=F32)


def tn(a, b):
    return lax.dot_general(a, b, (((0,), (0,)), ((), ())), preferred_element_type=F32)


def nn(a, b):
    return jnp.dot(a, b, preferred_element_type=F32)


def remote(src, dst, send, recv, dev):
    return pltpu.make_async_remote_copy(
        src_ref=src, dst_ref=dst, send_sem=send, recv_sem=recv, device_id=dev, device_id_type=MESH
    )


def loop(n, f, start=0):
    def step(i, c):
        f(i)
        return c

    lax.fori_loop(start, n, step, 0)


def column(row):
    n = row.shape[1]
    eye = lax.broadcasted_iota(jnp.int32, (n, n), 0) == lax.broadcasted_iota(jnp.int32, (n, n), 1)
    spread = jnp.where(eye, jnp.broadcast_to(row, (n, n)), jnp.zeros((n, n), row.dtype))
    return jnp.sum(spread, axis=1, keepdims=True)


def kernel(
    tok_hbm, og_hbm, prob_hbm, id_hbm, slot_hbm, wg_hbm, wu_hbm, wd_hbm,
    y_out, gg_out, gu_out, gd_out,
    tok, og, prob, ids, slots, wg, wu, wd, wgT, wuT, wdT, tab,
    sendA, recvA, sendC, recvC, XG, XT, part, rs1, raw, red, redS, H,
    rgp, recvP, qs, recvQ, zs, recvZ, sendY, recvY, accd,
    isem, wsem, sA, rA, sC, rC, sD, rD, sR, rR, sG, rG, sN, rN, sP, rP, sQ, rQ, sZ, rZ, sY, rY,
):
    d, e, t = lax.axis_index("dp"), lax.axis_index("expert"), lax.axis_index("tensor")
    b = d * 8 + e
    core, y = lax.rem(t, 2), lax.div(t, 2)
    mate = t + 1 - 2 * core
    right, left, opp = lax.rem(d + 1, 4), lax.rem(d + 3, 4), lax.rem(d + 2, 4)

    def at_t(tt):
        return (d, e, tt)

    def at_p(p):
        return (lax.div(p, 8), lax.rem(p, 8), t)

    def far_first(n):
        def swing(m):
            return lax.div(m + 1, 2) * (1 - 2 * lax.rem(m, 2))

        z = lax.rem(2 * d + lax.div(e, 4) + 4 + swing(lax.div(n, 4)) + 8, 8)
        x = lax.rem(lax.rem(e, 4) + 2 + swing(lax.rem(n, 4)) + 4, 4)
        return lax.div(z, 2) * 8 + lax.rem(z, 2) * 4 + x

    bar = pltpu.get_barrier_semaphore()

    def greet_t(k):
        pl.semaphore_signal(bar, inc=1, device_id=at_t(lax.rem(t + k, 8)), device_id_type=MESH)

    def greet_p(k):
        pl.semaphore_signal(bar, inc=1, device_id=at_p(far_first(k)), device_id_type=MESH)

    loop(31, greet_p)
    loop(8, greet_t, 1)

    inputs = [
        pltpu.make_async_copy(src, dst, isem.at[n])
        for n, (src, dst) in enumerate(
            ((tok_hbm, tok), (og_hbm, og), (prob_hbm, prob), (id_hbm, ids), (slot_hbm, slots))
        )
    ]
    weights = [
        pltpu.make_async_copy(src, dst, wsem.at[n])
        for n, (src, dst) in enumerate(((wg_hbm, wg), (wu_hbm, wu), (wd_hbm, wd)))
    ]
    for c in inputs + weights:
        c.start()
    for c in inputs:
        c.wait()
    for dd in range(4):
        for q in range(8):
            at = slice(1024 * dd + 128 * q, 1024 * dd + 128 * q + 128)
            sendA[q, 0, :, 128 * dd : 128 * dd + 128] = tok[:, at]
            sendA[q, 1, :, 128 * dd : 128 * dd + 128] = og[:, at]
    slot, owner = slots[...], ids[...] * 8
    place = jnp.where(
        slot >= 16,
        owner + 4 * lax.rem(e, 2) + slot - 16,
        jnp.where(slot < 8, 64 + owner + slot, 120 + owner + slot),
    )
    place = jnp.where(slot < CAP, place, -1)
    by_place = lax.broadcasted_iota(jnp.int32, (PLACES, 64), 0)
    t0, t1 = ((by_place == place[k : k + 1]).astype(F32) for k in range(2))
    tx, t0, t1 = (t0 + t1).astype(BF), t0.astype(BF), t1.astype(BF)
    by_token = lax.broadcasted_iota(jnp.int32, (64, PLACES), 1)
    tab[...] = sum((by_token == column(place[k : k + 1])).astype(F32) for k in range(2)).astype(BF)
    p0, p1 = (column(prob[k : k + 1]) for k in range(2))
    pl.semaphore_wait(bar, 38)

    def send_a(k):
        q = lax.rem(t + k, 8)
        return remote(sendA.at[q], recvA.at[t], sA.at[q], rA.at[t], at_t(q))

    loop(8, lambda k: send_a(k).start(), 1)
    recvA[t] = sendA[t]

    def wait_a(k):
        q = lax.rem(t + k, 8)
        remote(recvA.at[q], recvA.at[q], sA.at[q], rA.at[q], at_t(q)).wait_recv()

    loop(8, wait_a, 1)

    rx = recvA[:, 0].astype(F32).reshape(64, 512).astype(BF)
    ry = recvA[:, 1].astype(F32).reshape(64, 512)
    xb = nn(tx, rx)
    gb = nn(t0, (p0 * ry).astype(BF)) + nn(t1, (p1 * ry).astype(BF))
    for c in range(3):
        for dd in range(4):
            cut = slice(64 * c, 64 * c + 64), slice(128 * dd, 128 * dd + 128)
            for a, v in enumerate((xb, gb)):
                sendC[c, 8 * dd : 8 * dd + 8, a] = v[cut].reshape(8, 8, 128).astype(BF)

    def send_c(c, k):
        p = far_first(k)
        return remote(sendC.at[c, p], recvC.at[c, b], sC.at[c, p], rC.at[c, b], at_p(p))

    for c in range(3):
        loop(31, lambda k, c=c: send_c(c, k).start())
        recvC[c, b] = sendC[c, b]

    def wait_c(c, p):
        @pl.when(p != b)
        def _():
            ref = recvC.at[c, p]
            remote(ref, ref, sC.at[c, p], rC.at[c, p], at_p(p)).wait_recv()

    def piece(src, i):
        return XG.at[src, :, pl.ds(8 * i, 8)]

    def send_d(i, slot, src, dst):
        return remote(piece(src, i), piece(src, i), sD.at[i, slot], rD.at[i, src], at_t(dst))

    def wait_d(i, src):
        remote(piece(src, i), piece(src, i), sD.at[i, 0], rD.at[i, src], at_t(mate)).wait_recv()

    def octet(c, p, a):
        return recvC[c, p, a].astype(F32)

    def start_d(i):
        for k in (2, 1, 3):
            send_d(i, k, t, lax.rem(t + 2 * k, 8)).start()
        send_d(i, 0, t, mate).start()

    def relay_d(i):
        for k in (1, 3, 2):
            q = lax.rem(t + 2 * k, 8)
            wait_d(i, q)
            send_d(i, 4 + k, q, mate).start()

    def arrive_d(i):
        for k in range(4):
            wait_d(i, lax.rem(mate + 2 * k, 8))

    for c in weights:
        c.wait()

    def flip(src, dst):
        rows, cols = src.shape

        def one(r):
            at = pl.ds(pl.multiple_of(128 * r, 128), 128)
            for f in range(cols // 128):
                dst[128 * f : 128 * f + 128, at] = src[at, 128 * f : 128 * f + 128].T

        loop(rows // 128, one)

    flip(wd, wdT)
    loop(32, lambda p: wait_c(0, p))

    def rest(j):
        for a in range(2):
            lo = octet(0, 4 * j, a) + octet(0, 4 * j + 1, a)
            hi = octet(0, 4 * j + 2, a) + octet(0, 4 * j + 3, a)
            XG[t, a, j] = jnp.concatenate([lo, hi], axis=0).astype(BF)

    loop(8, rest)
    start_d(0)

    def prep(i):
        c, first = lax.div(i + 1, 2), 16 * lax.rem(i + 1, 2)

        def one(j):
            p = first + 2 * j
            wait_c(c, p)
            wait_c(c, p + 1)
            for a in range(2):
                both = jnp.concatenate([octet(c, p, a), octet(c, p + 1, a)], axis=0)
                XG[t, a, 8 * i + j] = both.astype(BF)

        loop(8, one)
        start_d(i)

    def tile(i, owner, half):
        return 8 * i + 2 * owner + half

    def peer(dd):
        return (dd, e, t)

    def rs_send(i, m):
        src, dst, dev = {
            0: (part.at[:, tile(i, opp, 0)], rs1.at[0, i], right),
            1: (part.at[:, tile(i, right, 1)], raw.at[0, i], right),
            2: (redS.at[0, i], red.at[0, i], right),
            3: (part.at[:, tile(i, opp, 1)], rs1.at[1, i], left),
            4: (part.at[:, tile(i, left, 0)], raw.at[1, i], left),
            5: (redS.at[1, i], red.at[1, i], left),
        }[m]
        return remote(src, dst, sR.at[i, m], rR.at[i, m], peer(dev))

    def rs_wait(i, m):
        dst = (rs1, raw, red)[m % 3].at[m // 3, i]
        remote(dst, dst, sR.at[i, m], rR.at[i, m], peer(right)).wait_recv()

    def rows_of(a, i):
        tiles = pl.ds(8 * i, 8)
        return jnp.concatenate([XG[q, a, tiles].reshape(128, 128) for q in range(8)], axis=1)

    def forward(i):
        tiles = pl.ds(8 * i, 8)
        xs = rows_of(0, i)
        part[0, tiles] = nn(xs, wg[...]).astype(BF).reshape(8, 16, -1)
        part[1, tiles] = nn(xs, wu[...]).astype(BF).reshape(8, 16, -1)
        part[2, tiles] = nn(rows_of(1, i), wdT[...]).astype(BF).reshape(8, 16, -1)
        for m in (0, 3, 1, 4):
            rs_send(i, m).start()

    def open_stage(i):
        @pl.when(i < S - 1)
        def _():
            prep(i + 1)

        relay_d(i)
        arrive_d(i)
        forward(i)

    loop(S, open_stage)
    flip(wg, wgT)
    flip(wu, wuT)

    def middle(i):
        rs_wait(i, 0)
        redS[0, i] = (part[:, tile(i, right, 0)].astype(F32) + rs1[0, i].astype(F32)).astype(BF)
        rs_send(i, 2).start()
        rs_wait(i, 3)
        redS[1, i] = (part[:, tile(i, left, 1)].astype(F32) + rs1[1, i].astype(F32)).astype(BF)
        rs_send(i, 5).start()

    loop(S, middle)

    def ag_ref(i, owner, half=None):
        return H.at[1:3, i, pl.ds(2 * owner, 2) if half is None else 2 * owner + half]

    def hid_ref(n, owner, half=None):
        return H.at[0, pl.ds(3 * n, 3 - n), pl.ds(2 * owner, 2) if half is None else 2 * owner + half]

    def ring(ref, i, m, sems):
        src, dev = {
            0: (ref(i, d), right), 1: (ref(i, d), left),
            2: (ref(i, left, 0), right), 3: (ref(i, right, 1), left),
        }[m]
        return remote(src, src, sems[0].at[i, m], sems[1].at[i, m], peer(dev))

    def ring_wait(ref, i, m, sems):
        dst = (ref(i, left), ref(i, right), ref(i, opp, 0), ref(i, opp, 1))[m]
        remote(dst, dst, sems[0].at[i, m], sems[1].at[i, m], peer(right)).wait_recv()

    def ag_send(i, m):
        return ring(ag_ref, i, m, (sG, rG))

    def ag_wait(i, m):
        ring_wait(ag_ref, i, m, (sG, rG))

    def hid_send(n, m):
        return ring(hid_ref, n, m, (sN, rN))

    def hid_wait(n, m):
        ring_wait(hid_ref, n, m, (sN, rN))

    def own(i):
        rs_wait(i, 1)
        rs_wait(i, 4)
        for half, (ra, rb, m) in enumerate(((red, raw, 2), (raw, red, 5))):
            rs_wait(i, m)
            at, to = tile(i, d, half), 2 * d + half
            gate, up, grad = (
                part[u, at].astype(F32) + ra[0, i, u].astype(F32) + rb[1, i, u].astype(F32)
                for u in range(3)
            )
            s = jax.nn.sigmoid(gate)
            silu = gate * s
            H[0, i, to] = (silu * up).astype(BF)
            H[1, i, to] = (grad * up * s * (1.0 + gate * (1.0 - s))).astype(BF)
            H[2, i, to] = (grad * silu).astype(BF)
        ag_send(i, 0).start()
        ag_send(i, 1).start()

    def relay(i):
        ag_wait(i, 0)
        ag_send(i, 2).start()
        ag_wait(i, 1)
        ag_send(i, 3).start()

    def p_copy(i):
        return remote(rgp.at[i, 1 - core], recvP.at[i], sP.at[i], rP.at[i], at_t(mate))

    def q_send(i, k):
        yy = lax.rem(y + k, 4)
        return remote(qs.at[i, yy], recvQ.at[i, y], sQ.at[i, yy], rQ.at[i, y], at_t(2 * yy + core))

    def hid(u, i):
        return H[u, i].reshape(128, -1)

    def rows(i):
        ag_wait(i, 2)
        ag_wait(i, 3)
        rg = nn(hid(1, i), wgT[...]) + nn(hid(2, i), wuT[...])
        for q in range(8):
            rgp[i, q % 2, q // 2] = rg[:, 128 * q : 128 * q + 128].astype(BF)
        p_copy(i).start()

    def pair(i):
        remote(recvP.at[i], recvP.at[i], sP.at[i], rP.at[i], at_t(mate)).wait_recv()
        qs[i] = (rgp[i, core].astype(F32) + recvP[i].astype(F32)).astype(BF)
        for k in (2, 1, 3):
            q_send(i, k).start()

    def z_main(i, o):
        c, p = lax.div(i + 1, 2), 16 * lax.rem(i + 1, 2) + o
        return c, p, remote(zs.at[i, o], recvZ.at[c, b], sZ.at[c, p], rZ.at[c, b], at_p(p))

    def z_rest(p):
        return remote(zs.at[0, lax.div(p, 2)], recvZ.at[0, b], sZ.at[0, p], rZ.at[0, b], at_p(p))

    def back(i):
        tot = qs[i, y].astype(F32)
        for k in (1, 3, 2):
            yy = lax.rem(y + k, 4)
            remote(recvQ.at[i, yy], recvQ.at[i, yy], sQ.at[i, yy], rQ.at[i, yy], at_t(mate)).wait_recv()
            tot = tot + recvQ[i, yy].astype(F32)
        zs[i] = tot.reshape(16, 8, 128).astype(BF)

        @pl.when(i > 0)
        def _():
            def one(o):
                c, p, copy = z_main(i, o)

                @pl.when(p != b)
                def _():
                    copy.start()

                @pl.when(p == b)
                def _():
                    recvZ[c, b] = zs[i, o]

            loop(16, one)

        @pl.when(i == 0)
        def _():
            loop(31, lambda k: z_rest(far_first(k)).start())
            recvZ[0, b] = zs[0, lax.div(b, 2)]

    def turn(i):
        for q in range(8):
            v = XG[q, 0, pl.ds(8 * i, 8)].reshape(128, 128)
            XT[128 * q : 128 * q + 128, pl.ds(pl.multiple_of(128 * i, 128), 128)] = v.T

    def model_grad(u, out):
        out[0] = nn(XT[...], H[u].reshape(640, -1)).astype(BF)

    def down_part(lo, hi):
        g = jnp.concatenate(
            [XG[q, 1, 8 * lo : 8 * hi].reshape(128 * (hi - lo), 128) for q in range(8)], axis=1
        )
        return tn(H[0, lo:hi].reshape(128 * (hi - lo), -1), g)

    loop(S, turn)
    own(0)
    own(1)
    relay(0)

    def cycle(i):
        @pl.when(i + 2 < S)
        def _():
            own(i + 2)

        @pl.when(i + 1 < S)
        def _():
            relay(i + 1)

        @pl.when(i == S - 2)
        def _():
            for m in (0, 1):
                hid_send(0, m).start()

        @pl.when(i >= 1)
        def _():
            pair(i - 1)

        @pl.when(i >= 2)
        def _():
            back(i - 2)

        rows(i)

    loop(S, cycle)
    pair(S - 1)
    back(S - 2)
    model_grad(1, gg_out)
    back(S - 1)
    for m in (0, 1):
        hid_send(1, m).start()

    def hid_relay(n):
        for m in (0, 1):
            hid_wait(n, m)
            hid_send(n, m + 2).start()

    hid_relay(0)
    model_grad(2, gu_out)
    hid_relay(1)

    def wait_z(k):
        p = lax.rem(b + k, 32)
        for c in range(3):
            ref = recvZ.at[c, p]
            remote(ref, ref, sZ.at[c, p], rZ.at[c, p], at_p(p)).wait_recv()

    loop(32, wait_z, 1)
    for dd in range(4):
        z = recvZ[:, 8 * dd : 8 * dd + 8].astype(F32).reshape(PLACES, 128).astype(BF)
        part_rows = nn(tab[...], z).reshape(8, 8, 128).astype(BF)
        sendY[:, :, 128 * dd : 128 * dd + 128] = part_rows

    def y_copy(k):
        q = lax.rem(t + k, 8)
        return remote(sendY.at[q], recvY.at[t], sY.at[q], rY.at[t], at_t(q))

    loop(8, lambda k: y_copy(k).start(), 1)
    recvY[t] = sendY[t]
    for m in (2, 3):
        hid_wait(0, m)
    accd[...] = down_part(0, 3)

    loop(8, lambda k: send_a(k).wait_send(), 1)
    for c in range(3):
        loop(31, lambda k, c=c: send_c(c, k).wait_send())

    def drain(i):
        for k in range(4):
            send_d(i, k, t, mate).wait_send()
        for k in range(1, 4):
            send_d(i, 4 + k, t, mate).wait_send()
            q_send(i, k).wait_send()
        for m in range(6):
            rs_send(i, m).wait_send()
        for m in range(4):
            ag_send(i, m).wait_send()
        p_copy(i).wait_send()

        @pl.when(i > 0)
        def _():
            def one(o):
                c, p, copy = z_main(i, o)

                @pl.when(p != b)
                def _():
                    copy.wait_send()

            loop(16, one)

    loop(S, drain)
    loop(31, lambda k: z_rest(far_first(k)).wait_send())

    def wait_y(k):
        q = lax.rem(t + k, 8)
        remote(recvY.at[q], recvY.at[q], sY.at[q], rY.at[q], at_t(q)).wait_recv()

    loop(8, wait_y, 1)
    for dd in range(4):
        for q in range(8):
            at = slice(1024 * dd + 128 * q, 1024 * dd + 128 * q + 128)
            y_out[:, at] = recvY[q, :, 128 * dd : 128 * dd + 128]
    loop(8, lambda k: y_copy(k).wait_send(), 1)
    for m in (2, 3):
        hid_wait(1, m)
    gd_out[0] = (accd[...] + down_part(3, S)).astype(BF)
    for n in (0, 1):
        for m in range(4):
            hid_send(n, m).wait_send()


def shards(tokens, out_grad, route_probs, expert_ids, slot_index, w_gate, w_up, w_down):
    wg, wu, wd = w_gate[0], w_up[0], w_down[0]
    dl, fl = wg.shape
    vm = pl.BlockSpec(memory_space=pltpu.VMEM)
    hbm = pl.BlockSpec(memory_space=pl.ANY)
    dma = pltpu.SemaphoreType.DMA

    def buf(*shape, dtype=BF):
        return pltpu.VMEM(shape, dtype)

    yv, gg, gu, gd = pl.pallas_call(
        kernel,
        name="expert_back",
        out_shape=(
            jax.ShapeDtypeStruct(tokens.shape, BF),
            jax.ShapeDtypeStruct(w_gate.shape, BF),
            jax.ShapeDtypeStruct(w_up.shape, BF),
            jax.ShapeDtypeStruct(w_down.shape, BF),
        ),
        in_specs=[hbm] * 8,
        out_specs=(vm, vm, vm, vm),
        scratch_shapes=[
            buf(8, 4096), buf(8, 4096), buf(2, 64, dtype=F32),
            buf(2, 64, dtype=jnp.int32), buf(2, 64, dtype=jnp.int32),
            buf(dl, fl), buf(dl, fl), buf(fl, dl), buf(fl, dl), buf(fl, dl), buf(dl, fl), buf(64, PLACES),
            buf(8, 2, 8, 512), buf(8, 2, 8, 512),
            buf(3, 32, 2, 8, 128), buf(3, 32, 2, 8, 128),
            buf(8, 2, 40, 16, 128), buf(dl, 640), buf(3, 40, 16, fl),
            buf(2, S, 3, 16, fl), buf(2, S, 3, 16, fl), buf(2, S, 3, 16, fl), buf(2, S, 3, 16, fl),
            buf(3, S, 8, 16, fl),
            buf(S, 2, 4, 128, 128), buf(S, 4, 128, 128), buf(S, 4, 128, 128), buf(S, 4, 128, 128),
            buf(S, 16, 8, 128), buf(3, 32, 8, 128), buf(8, 8, 512), buf(8, 8, 512),
            buf(fl, dl, dtype=F32),
            dma((5,)), dma((3,)), dma((8,)), dma((8,)), dma((3, 32)), dma((3, 32)),
            dma((S, 8)), dma((S, 8)), dma((S, 6)), dma((S, 6)), dma((S, 4)), dma((S, 4)),
            dma((2, 4)), dma((2, 4)), dma((S,)), dma((S,)), dma((S, 4)), dma((S, 4)), dma((3, 32)), dma((3, 32)),
            dma((8,)), dma((8,)),
        ],
        compiler_params=pltpu.CompilerParams(
            collective_id=0, has_side_effects=True, vmem_limit_bytes=48 * 1024 * 1024
        ),
    )(tokens, out_grad, route_probs.T, expert_ids.T, slot_index.T, wg, wu, wd)
    return yv, gg, gu, gd


def solution(mesh):
    placed = (
        P(("dp", "expert", "tensor"), None),
        P(("dp", "expert", "tensor"), None),
        P(("dp", "expert"), None),
        P(("dp", "expert"), None),
        P(("dp", "expert"), None),
        P("expert", "dp", "tensor"),
        P("expert", "dp", "tensor"),
        P("expert", "tensor", "dp"),
    )
    return jax.shard_map(
        shards,
        mesh=mesh,
        in_specs=placed,
        out_specs=(
            P(("dp", "expert", "tensor"), None),
            P("expert", "dp", "tensor"),
            P("expert", "dp", "tensor"),
            P("expert", "tensor", "dp"),
        ),
        check_vma=False,
    )
```

```python
import jax
import jax.numpy as jnp
from jax import lax
from jax.experimental import pallas as pl
from jax.experimental.pallas import tpu as pltpu
from jax.sharding import PartitionSpec as P

BF, F32 = jnp.bfloat16, jnp.float32
MESH = pl.DeviceIdType.MESH
S = 5
CAP = 20
PLACES = 192


def nt(a, b):
    return lax.dot_general(a, b, (((1,), (1,)), ((), ())), preferred_element_type=F32)


def tn(a, b):
    return lax.dot_general(a, b, (((0,), (0,)), ((), ())), preferred_element_type=F32)


def nn(a, b):
    return jnp.dot(a, b, preferred_element_type=F32)


def remote(src, dst, send, recv, dev):
    return pltpu.make_async_remote_copy(
        src_ref=src, dst_ref=dst, send_sem=send, recv_sem=recv, device_id=dev, device_id_type=MESH
    )


def loop(n, f, start=0):
    def step(i, c):
        f(i)
        return c

    lax.fori_loop(start, n, step, 0)


def column(row):
    n = row.shape[1]
    eye = lax.broadcasted_iota(jnp.int32, (n, n), 0) == lax.broadcasted_iota(jnp.int32, (n, n), 1)
    spread = jnp.where(eye, jnp.broadcast_to(row, (n, n)), jnp.zeros((n, n), row.dtype))
    return jnp.sum(spread, axis=1, keepdims=True)


def kernel(
    tok_hbm, og_hbm, prob_hbm, id_hbm, slot_hbm, wg_hbm, wu_hbm, wd_hbm,
    y_out, gg_out, gu_out, gd_out,
    tok, og, prob, ids, slots, wg, wu, wd, wgT, wuT, wdT, tab,
    sendA, recvA, sendR, recvR, sendC, recvC, XG, XT, part, rs1, raw, red, redS, H,
    rgp, recvP, qs, recvQ, zs, recvZ, sendY, recvY, accd,
    isem, wsem, sA, rA, sL, rL, sC, rC, sD, rD, sR, rR, sG, rG, sN, rN, sP, rP, sQ, rQ, sZ, rZ, sY, rY,
):
    d, e, t = lax.axis_index("dp"), lax.axis_index("expert"), lax.axis_index("tensor")
    b = d * 8 + e
    core, y = lax.rem(t, 2), lax.div(t, 2)
    mate = t + 1 - 2 * core
    right, left, opp = lax.rem(d + 1, 4), lax.rem(d + 3, 4), lax.rem(d + 2, 4)

    def at_t(tt):
        return (d, e, tt)

    def at_p(p):
        return (lax.div(p, 8), lax.rem(p, 8), t)

    def far_first(n):
        def swing(m):
            return lax.div(m + 1, 2) * (1 - 2 * lax.rem(m, 2))

        z = lax.rem(2 * d + lax.div(e, 4) + 4 + swing(lax.div(n, 4)) + 8, 8)
        x = lax.rem(lax.rem(e, 4) + 2 + swing(lax.rem(n, 4)) + 4, 4)
        return lax.div(z, 2) * 8 + lax.rem(z, 2) * 4 + x

    bar = pltpu.get_barrier_semaphore()

    def greet_t(k):
        pl.semaphore_signal(bar, inc=1, device_id=at_t(lax.rem(t + k, 8)), device_id_type=MESH)

    def greet_p(k):
        pl.semaphore_signal(bar, inc=1, device_id=at_p(far_first(k)), device_id_type=MESH)

    loop(31, greet_p)
    loop(8, greet_t, 1)

    inputs = [
        pltpu.make_async_copy(src, dst, isem.at[n])
        for n, (src, dst) in enumerate(
            ((tok_hbm, tok), (og_hbm, og), (prob_hbm, prob), (id_hbm, ids), (slot_hbm, slots))
        )
    ]
    weights = [
        pltpu.make_async_copy(src, dst, wsem.at[n])
        for n, (src, dst) in enumerate(((wg_hbm, wg), (wu_hbm, wu), (wd_hbm, wd)))
    ]
    for c in inputs + weights:
        c.start()
    for c in inputs:
        c.wait()
    for dd in range(4):
        for q in range(8):
            at = slice(1024 * dd + 128 * q, 1024 * dd + 128 * q + 128)
            sendA[q, 0, :, 128 * dd : 128 * dd + 128] = tok[:, at]
            sendA[q, 1, :, 128 * dd : 128 * dd + 128] = og[:, at]
    slot, owner = slots[...], ids[...] * 8
    past = slot >= 16
    low = jnp.where(slot < 8, 64 + owner + slot, 120 + owner + slot)

    def places(extra):
        return jnp.where(slot < CAP, jnp.where(past, owner + slot - 16 + extra, low), -1)

    place_x, place_g, place_z = places(0), places(4), places(4 * lax.rem(e, 2))
    by_place = lax.broadcasted_iota(jnp.int32, (PLACES, 64), 0)
    tx = sum((by_place == place_x[k : k + 1]).astype(F32) for k in range(2)).astype(BF)
    t0, t1 = ((by_place == place_g[k : k + 1]).astype(BF) for k in range(2))
    by_token = lax.broadcasted_iota(jnp.int32, (64, PLACES), 1)
    tab[...] = sum((by_token == column(place_z[k : k + 1])).astype(F32) for k in range(2)).astype(BF)
    p0, p1 = (column(prob[k : k + 1]) for k in range(2))
    pl.semaphore_wait(bar, 38)

    def send_a(k):
        q = lax.rem(t + k, 8)
        return remote(sendA.at[q], recvA.at[t], sA.at[q], rA.at[t], at_t(q))

    loop(8, lambda k: send_a(k).start(), 1)
    recvA[t] = sendA[t]

    def wait_a(k):
        q = lax.rem(t + k, 8)
        remote(recvA.at[q], recvA.at[q], sA.at[q], rA.at[q], at_t(q)).wait_recv()

    loop(8, wait_a, 1)

    rx = recvA[:, 0].astype(F32).reshape(64, 512).astype(BF)
    ry = recvA[:, 1].astype(F32).reshape(64, 512)
    xb = nn(tx, rx)
    gb = nn(t0, (p0 * ry).astype(BF)) + nn(t1, (p1 * ry).astype(BF))
    for dd in range(4):
        cols, to = slice(128 * dd, 128 * dd + 128), slice(8 * dd, 8 * dd + 8)
        sendR[to] = (xb[:64, cols] + gb[:64, cols]).reshape(8, 8, 128).astype(BF)
        for c in range(2):
            for a, v in enumerate((xb, gb)):
                sendC[c, to, a] = v[64 * c + 64 : 64 * c + 128, cols].reshape(8, 8, 128).astype(BF)

    def send_l(k):
        p = far_first(k)
        return remote(sendR.at[p], recvR.at[b], sL.at[p], rL.at[b], at_p(p))

    def send_c(c, k):
        p = far_first(k)
        return remote(sendC.at[c, p], recvC.at[c, b], sC.at[c, p], rC.at[c, b], at_p(p))

    loop(31, lambda k: send_l(k).start())
    recvR[b] = sendR[b]
    for c in range(2):
        loop(31, lambda k, c=c: send_c(c, k).start())
        recvC[c, b] = sendC[c, b]

    def wait_l(p):
        @pl.when(p != b)
        def _():
            remote(recvR.at[p], recvR.at[p], sL.at[p], rL.at[p], at_p(p)).wait_recv()

    def wait_c(c, p):
        @pl.when(p != b)
        def _():
            ref = recvC.at[c, p]
            remote(ref, ref, sC.at[c, p], rC.at[c, p], at_p(p)).wait_recv()

    def piece(src, a, i):
        return XG.at[src, a, pl.ds(8 * i, 8)]

    def send_d(i, a, slot, src, dst):
        ref = piece(src, a, i)
        return remote(ref, ref, sD.at[i, a, slot], rD.at[i, a, src], at_t(dst))

    def wait_d(i, a, src):
        ref = piece(src, a, i)
        remote(ref, ref, sD.at[i, a, 0], rD.at[i, a, src], at_t(mate)).wait_recv()

    def octet(c, p, a):
        return recvC[c, p, a].astype(F32)

    def start_d(i):
        for a in range(2):
            for k in (2, 1, 3):
                send_d(i, a, k, t, lax.rem(t + 2 * k, 8)).start()
            send_d(i, a, 0, t, mate).start()

    def relay_d(i, a):
        for k in (1, 3, 2):
            q = lax.rem(t + 2 * k, 8)
            wait_d(i, a, q)
            send_d(i, a, 4 + k, q, mate).start()

    def arrive_d(i, a):
        for k in range(4):
            wait_d(i, a, lax.rem(mate + 2 * k, 8))

    for c in weights:
        c.wait()

    def flip(src, dst):
        rows, cols = src.shape

        def one(r):
            at = pl.ds(pl.multiple_of(128 * r, 128), 128)
            for f in range(cols // 128):
                dst[128 * f : 128 * f + 128, at] = src[at, 128 * f : 128 * f + 128].T

        loop(rows // 128, one)

    flip(wd, wdT)
    loop(32, wait_l)

    def rest(j):
        four = [recvR[4 * j + q].astype(F32) for q in range(4)]
        for a in range(2):
            XG[t, a, j] = jnp.concatenate([v[4 * a : 4 * a + 4] for v in four], axis=0).astype(BF)

    loop(8, rest)
    start_d(0)

    def prep(i):
        c, first = lax.div(i - 1, 2), 16 * lax.rem(i + 1, 2)

        def one(j):
            p = first + 2 * j
            wait_c(c, p)
            wait_c(c, p + 1)
            for a in range(2):
                both = jnp.concatenate([octet(c, p, a), octet(c, p + 1, a)], axis=0)
                XG[t, a, 8 * i + j] = both.astype(BF)

        loop(8, one)
        start_d(i)

    def tile(i, owner, half):
        return 8 * i + 2 * owner + half

    def peer(dd):
        return (dd, e, t)

    UNITS = (slice(0, 2), slice(2, 3), slice(0, 3))

    def rs_send(i, m, w=2):
        u = UNITS[w]
        src, dst, dev = {
            0: (part.at[u, tile(i, opp, 0)], rs1.at[0, i, u], right),
            1: (part.at[u, tile(i, right, 1)], raw.at[0, i, u], right),
            2: (redS.at[0, i], red.at[0, i], right),
            3: (part.at[u, tile(i, opp, 1)], rs1.at[1, i, u], left),
            4: (part.at[u, tile(i, left, 0)], raw.at[1, i, u], left),
            5: (redS.at[1, i], red.at[1, i], left),
        }[m]
        return remote(src, dst, sR.at[i, m, w % 2], rR.at[i, m, w % 2], peer(dev))

    def rs_wait(i, m):
        for w in (2,) if m % 3 == 2 else (0, 1):
            dst = (rs1, raw, red)[m % 3].at[m // 3, i, UNITS[w]]
            remote(dst, dst, sR.at[i, m, w % 2], rR.at[i, m, w % 2], peer(right)).wait_recv()

    def rs_sends(i):
        return [rs_send(i, m, w) for m in (0, 1, 3, 4) for w in (0, 1)] + [rs_send(i, 2), rs_send(i, 5)]

    def rows_of(a, i):
        tiles = pl.ds(8 * i, 8)
        return jnp.concatenate([XG[q, a, tiles].reshape(128, 128) for q in range(8)], axis=1)

    def forward(i):
        tiles = pl.ds(8 * i, 8)
        relay_d(i, 0)
        arrive_d(i, 0)
        xs = rows_of(0, i)
        part[0, tiles] = nn(xs, wg[...]).astype(BF).reshape(8, 16, -1)
        part[1, tiles] = nn(xs, wu[...]).astype(BF).reshape(8, 16, -1)
        for m in (0, 3, 1, 4):
            rs_send(i, m, 0).start()
        relay_d(i, 1)
        arrive_d(i, 1)
        part[2, tiles] = nn(rows_of(1, i), wdT[...]).astype(BF).reshape(8, 16, -1)
        for m in (0, 3, 1, 4):
            rs_send(i, m, 1).start()

    def open_stage(i):
        @pl.when(i < S - 1)
        def _():
            prep(i + 1)

        forward(i)

    loop(S, open_stage)
    flip(wg, wgT)
    flip(wu, wuT)

    def middle(i):
        rs_wait(i, 0)
        redS[0, i] = (part[:, tile(i, right, 0)].astype(F32) + rs1[0, i].astype(F32)).astype(BF)
        rs_send(i, 2).start()
        rs_wait(i, 3)
        redS[1, i] = (part[:, tile(i, left, 1)].astype(F32) + rs1[1, i].astype(F32)).astype(BF)
        rs_send(i, 5).start()

    loop(S, middle)

    HID = (slice(0, 3), slice(3, 4), slice(4, 5))

    def ag_ref(i, owner, half=None):
        return H.at[1:3, i, pl.ds(2 * owner, 2) if half is None else 2 * owner + half]

    def hid_ref(n, owner, half=None):
        return H.at[0, HID[n], pl.ds(2 * owner, 2) if half is None else 2 * owner + half]

    def ring(ref, i, m, sems):
        src, dev = {
            0: (ref(i, d), right), 1: (ref(i, d), left),
            2: (ref(i, left, 0), right), 3: (ref(i, right, 1), left),
        }[m]
        return remote(src, src, sems[0].at[i, m], sems[1].at[i, m], peer(dev))

    def ring_wait(ref, i, m, sems):
        dst = (ref(i, left), ref(i, right), ref(i, opp, 0), ref(i, opp, 1))[m]
        remote(dst, dst, sems[0].at[i, m], sems[1].at[i, m], peer(right)).wait_recv()

    def ag_send(i, m):
        return ring(ag_ref, i, m, (sG, rG))

    def ag_wait(i, m):
        ring_wait(ag_ref, i, m, (sG, rG))

    def hid_send(n, m):
        return ring(hid_ref, n, m, (sN, rN))

    def hid_wait(n, m):
        ring_wait(hid_ref, n, m, (sN, rN))

    def own(i):
        rs_wait(i, 1)
        rs_wait(i, 4)
        for half, (ra, rb, m) in enumerate(((red, raw, 2), (raw, red, 5))):
            rs_wait(i, m)
            at, to = tile(i, d, half), 2 * d + half
            gate, up, grad = (
                part[u, at].astype(F32) + ra[0, i, u].astype(F32) + rb[1, i, u].astype(F32)
                for u in range(3)
            )
            s = jax.nn.sigmoid(gate)
            silu = gate * s
            H[0, i, to] = (silu * up).astype(BF)
            H[1, i, to] = (grad * up * s * (1.0 + gate * (1.0 - s))).astype(BF)
            H[2, i, to] = (grad * silu).astype(BF)
        ag_send(i, 0).start()
        ag_send(i, 1).start()

    def relay(i):
        ag_wait(i, 0)
        ag_send(i, 2).start()
        ag_wait(i, 1)
        ag_send(i, 3).start()

    def p_copy(i):
        return remote(rgp.at[i, 1 - core], recvP.at[i], sP.at[i], rP.at[i], at_t(mate))

    def q_send(i, k):
        yy = lax.rem(y + k, 4)
        return remote(qs.at[i, yy], recvQ.at[i, y], sQ.at[i, yy], rQ.at[i, y], at_t(2 * yy + core))

    def hid(u, i):
        return H[u, i].reshape(128, -1)

    def rows(i):
        ag_wait(i, 2)
        ag_wait(i, 3)
        rg = nn(hid(1, i), wgT[...]) + nn(hid(2, i), wuT[...])
        for q in range(8):
            rgp[i, q % 2, q // 2] = rg[:, 128 * q : 128 * q + 128].astype(BF)
        p_copy(i).start()

    def pair(i):
        remote(recvP.at[i], recvP.at[i], sP.at[i], rP.at[i], at_t(mate)).wait_recv()
        qs[i] = (rgp[i, core].astype(F32) + recvP[i].astype(F32)).astype(BF)
        for k in (2, 1, 3):
            q_send(i, k).start()

    def z_main(i, o):
        c, p = lax.div(i + 1, 2), 16 * lax.rem(i + 1, 2) + o
        return c, p, remote(zs.at[i, o], recvZ.at[c, b], sZ.at[c, p], rZ.at[c, b], at_p(p))

    def z_rest(p):
        return remote(zs.at[0, lax.div(p, 2)], recvZ.at[0, b], sZ.at[0, p], rZ.at[0, b], at_p(p))

    def back(i):
        tot = qs[i, y].astype(F32)
        for k in (1, 3, 2):
            yy = lax.rem(y + k, 4)
            remote(recvQ.at[i, yy], recvQ.at[i, yy], sQ.at[i, yy], rQ.at[i, yy], at_t(mate)).wait_recv()
            tot = tot + recvQ[i, yy].astype(F32)
        zs[i] = tot.reshape(16, 8, 128).astype(BF)

        @pl.when(i > 0)
        def _():
            def one(o):
                c, p, copy = z_main(i, o)

                @pl.when(p != b)
                def _():
                    copy.start()

                @pl.when(p == b)
                def _():
                    recvZ[c, b] = zs[i, o]

            loop(16, one)

        @pl.when(i == 0)
        def _():
            loop(31, lambda k: z_rest(far_first(k)).start())
            recvZ[0, b] = zs[0, lax.div(b, 2)]

    def turn(i):
        for q in range(8):
            v = XG[q, 0, pl.ds(8 * i, 8)].reshape(128, 128)
            XT[128 * q : 128 * q + 128, pl.ds(pl.multiple_of(128 * i, 128), 128)] = v.T

    def model_grad(u, out):
        out[0] = nn(XT[...], H[u].reshape(640, -1)).astype(BF)

    def down_part(lo, hi):
        g = jnp.concatenate(
            [XG[q, 1, 8 * lo : 8 * hi].reshape(128 * (hi - lo), 128) for q in range(8)], axis=1
        )
        return tn(H[0, lo:hi].reshape(128 * (hi - lo), -1), g)

    loop(S, turn)
    own(0)
    own(1)
    own(2)
    relay(0)

    def cycle(i):
        @pl.when(i + 3 < S)
        def _():
            own(i + 3)

        @pl.when(i + 1 < S)
        def _():
            relay(i + 1)

        @pl.when(i == S - 2)
        def _():
            for m in (0, 1):
                hid_send(0, m).start()

        @pl.when(i >= 1)
        def _():
            pair(i - 1)

        @pl.when(i >= 2)
        def _():
            back(i - 2)

        rows(i)

    loop(S, cycle)
    pair(S - 1)
    back(S - 2)
    model_grad(1, gg_out)
    back(S - 1)
    for n in (1, 2):
        for m in (0, 1):
            hid_send(n, m).start()

    def hid_relay(n):
        for m in (0, 1):
            hid_wait(n, m)
            hid_send(n, m + 2).start()

    hid_relay(0)
    model_grad(2, gu_out)
    hid_relay(1)
    hid_relay(2)

    def wait_z(k):
        p = lax.rem(b + k, 32)
        for c in range(3):
            ref = recvZ.at[c, p]
            remote(ref, ref, sZ.at[c, p], rZ.at[c, p], at_p(p)).wait_recv()

    loop(32, wait_z, 1)
    for dd in range(4):
        z = recvZ[:, 8 * dd : 8 * dd + 8].astype(F32).reshape(PLACES, 128).astype(BF)
        part_rows = nn(tab[...], z).reshape(8, 8, 128).astype(BF)
        sendY[:, :, 128 * dd : 128 * dd + 128] = part_rows

    def y_copy(k):
        q = lax.rem(t + k, 8)
        return remote(sendY.at[q], recvY.at[t], sY.at[q], rY.at[t], at_t(q))

    loop(8, lambda k: y_copy(k).start(), 1)
    recvY[t] = sendY[t]
    for n in (0, 1):
        for m in (2, 3):
            hid_wait(n, m)
    accd[...] = down_part(0, 4)

    loop(8, lambda k: send_a(k).wait_send(), 1)
    loop(31, lambda k: send_l(k).wait_send())
    for c in range(2):
        loop(31, lambda k, c=c: send_c(c, k).wait_send())

    def drain(i):
        for a in range(2):
            for k in (0, 1, 2, 3, 5, 6, 7):
                send_d(i, a, k, t, mate).wait_send()
        for k in range(1, 4):
            q_send(i, k).wait_send()
        for c in rs_sends(i):
            c.wait_send()
        for m in range(4):
            ag_send(i, m).wait_send()
        p_copy(i).wait_send()

        @pl.when(i > 0)
        def _():
            def one(o):
                c, p, copy = z_main(i, o)

                @pl.when(p != b)
                def _():
                    copy.wait_send()

            loop(16, one)

    loop(S, drain)
    loop(31, lambda k: z_rest(far_first(k)).wait_send())

    def wait_y(k):
        q = lax.rem(t + k, 8)
        remote(recvY.at[q], recvY.at[q], sY.at[q], rY.at[q], at_t(q)).wait_recv()

    loop(8, wait_y, 1)
    for dd in range(4):
        for q in range(8):
            at = slice(1024 * dd + 128 * q, 1024 * dd + 128 * q + 128)
            y_out[:, at] = recvY[q, :, 128 * dd : 128 * dd + 128]
    loop(8, lambda k: y_copy(k).wait_send(), 1)
    for m in (2, 3):
        hid_wait(2, m)
    gd_out[0] = (accd[...] + down_part(4, S)).astype(BF)
    for n in range(3):
        for m in range(4):
            hid_send(n, m).wait_send()


def put_out(*refs):
    sems = refs[8]
    copies = [pltpu.make_async_copy(refs[n], refs[4 + n], sems.at[n]) for n in range(4)]
    for c in copies:
        c.start()
    for c in copies:
        c.wait()


def shards(tokens, out_grad, route_probs, expert_ids, slot_index, w_gate, w_up, w_down):
    wg, wu, wd = w_gate[0], w_up[0], w_down[0]
    dl, fl = wg.shape
    vm = pl.BlockSpec(memory_space=pltpu.VMEM)
    hbm = pl.BlockSpec(memory_space=pl.ANY)
    dma = pltpu.SemaphoreType.DMA

    def buf(*shape, dtype=BF):
        return pltpu.VMEM(shape, dtype)

    yv, gg, gu, gd = pl.pallas_call(
        kernel,
        name="expert_back",
        out_shape=(
            jax.ShapeDtypeStruct(tokens.shape, BF),
            jax.ShapeDtypeStruct(w_gate.shape, BF),
            jax.ShapeDtypeStruct(w_up.shape, BF),
            jax.ShapeDtypeStruct(w_down.shape, BF),
        ),
        in_specs=[hbm] * 8,
        out_specs=(vm, vm, vm, vm),
        scratch_shapes=[
            buf(8, 4096), buf(8, 4096), buf(2, 64, dtype=F32),
            buf(2, 64, dtype=jnp.int32), buf(2, 64, dtype=jnp.int32),
            buf(dl, fl), buf(dl, fl), buf(fl, dl), buf(fl, dl), buf(fl, dl), buf(dl, fl), buf(64, PLACES),
            buf(8, 2, 8, 512), buf(8, 2, 8, 512),
            buf(32, 8, 128), buf(32, 8, 128), buf(2, 32, 2, 8, 128), buf(2, 32, 2, 8, 128),
            buf(8, 2, 40, 16, 128), buf(dl, 640), buf(3, 40, 16, fl),
            buf(2, S, 3, 16, fl), buf(2, S, 3, 16, fl), buf(2, S, 3, 16, fl), buf(2, S, 3, 16, fl),
            buf(3, S, 8, 16, fl),
            buf(S, 2, 4, 128, 128), buf(S, 4, 128, 128), buf(S, 4, 128, 128), buf(S, 4, 128, 128),
            buf(S, 16, 8, 128), buf(3, 32, 8, 128), buf(8, 8, 512), buf(8, 8, 512),
            buf(fl, dl, dtype=F32),
            dma((5,)), dma((3,)), dma((8,)), dma((8,)), dma((32,)), dma((32,)), dma((2, 32)), dma((2, 32)),
            dma((S, 2, 8)), dma((S, 2, 8)), dma((S, 6, 2)), dma((S, 6, 2)), dma((S, 4)), dma((S, 4)),
            dma((3, 4)), dma((3, 4)), dma((S,)), dma((S,)), dma((S, 4)), dma((S, 4)), dma((3, 32)), dma((3, 32)),
            dma((8,)), dma((8,)),
        ],
        compiler_params=pltpu.CompilerParams(
            collective_id=0, has_side_effects=True, vmem_limit_bytes=48 * 1024 * 1024
        ),
    )(*(
        pltpu.with_memory_space_constraint(v, pltpu.HBM)
        for v in (tokens, out_grad, route_probs.T, expert_ids.T, slot_index.T, wg, wu, wd)
    ))
    return pl.pallas_call(
        put_out,
        name="put_out",
        out_shape=tuple(jax.ShapeDtypeStruct(v.shape, v.dtype) for v in (yv, gg, gu, gd)),
        in_specs=[hbm] * 4,
        out_specs=(hbm,) * 4,
        scratch_shapes=[dma((4,))],
        compiler_params=pltpu.CompilerParams(vmem_limit_bytes=1024 * 1024),
    )(yv, gg, gu, gd)


def solution(mesh):
    placed = (
        P(("dp", "expert", "tensor"), None),
        P(("dp", "expert", "tensor"), None),
        P(("dp", "expert"), None),
        P(("dp", "expert"), None),
        P(("dp", "expert"), None),
        P("expert", "dp", "tensor"),
        P("expert", "dp", "tensor"),
        P("expert", "tensor", "dp"),
    )
    return jax.shard_map(
        shards,
        mesh=mesh,
        in_specs=placed,
        out_specs=(
            P(("dp", "expert", "tensor"), None),
            P("expert", "dp", "tensor"),
            P("expert", "dp", "tensor"),
            P("expert", "tensor", "dp"),
        ),
        check_vma=False,
    )
```

```python
import jax
import jax.numpy as jnp
from jax import lax
from jax.experimental import pallas as pl
from jax.experimental.pallas import tpu as pltpu
from jax.sharding import PartitionSpec as P

BF, F32 = jnp.bfloat16, jnp.float32
MESH = pl.DeviceIdType.MESH
S = 5
CAP = 20
PLACES = 192


def nt(a, b):
    return lax.dot_general(a, b, (((1,), (1,)), ((), ())), preferred_element_type=F32)


def tn(a, b):
    return lax.dot_general(a, b, (((0,), (0,)), ((), ())), preferred_element_type=F32)


def nn(a, b):
    return jnp.dot(a, b, preferred_element_type=F32)


def remote(src, dst, send, recv, dev):
    return pltpu.make_async_remote_copy(
        src_ref=src, dst_ref=dst, send_sem=send, recv_sem=recv, device_id=dev, device_id_type=MESH
    )


def loop(n, f, start=0):
    def step(i, c):
        f(i)
        return c

    lax.fori_loop(start, n, step, 0)


def column(row):
    n = row.shape[1]
    eye = lax.broadcasted_iota(jnp.int32, (n, n), 0) == lax.broadcasted_iota(jnp.int32, (n, n), 1)
    spread = jnp.where(eye, jnp.broadcast_to(row, (n, n)), jnp.zeros((n, n), row.dtype))
    return jnp.sum(spread, axis=1, keepdims=True)


def kernel(
    tok_hbm, og_hbm, prob_hbm, id_hbm, slot_hbm, wg_hbm, wu_hbm, wd_hbm,
    y_out, gg_out, gu_out, gd_out,
    tok, og, prob, ids, slots, wg, wu, wd, wgT, wuT, wdT, tab,
    sendA, recvA, sendR, recvR, sendC, recvC, XG, XT, part, rs1, raw, red, redS, H,
    rgp, recvP, qs, recvQ, zs, recvZ, sendY, recvY, accd,
    isem, wsem, one, rC, rD, rR, rG, rN, rP, rQ,
):
    d, e, t = lax.axis_index("dp"), lax.axis_index("expert"), lax.axis_index("tensor")
    b = d * 8 + e
    core, y = lax.rem(t, 2), lax.div(t, 2)
    mate = t + 1 - 2 * core
    right, left, opp = lax.rem(d + 1, 4), lax.rem(d + 3, 4), lax.rem(d + 2, 4)

    sA, rA, sL, rL, sC, sD, sR1, sRaw, sRed, sG, sN, sP, sQ, sZ, rZ, sY, rY = (
        one.at[n] for n in range(17)
    )

    def at_t(tt):
        return (d, e, tt)

    def got(ref, sem):
        remote(ref, ref, sem, sem, (d, e, mate)).wait_recv()

    def sent(ref, sem):
        remote(ref, ref, sem, sem, (d, e, mate)).wait_send()

    def at_p(p):
        return (lax.div(p, 8), lax.rem(p, 8), t)

    def far_first(n):
        def swing(m):
            return lax.div(m + 1, 2) * (1 - 2 * lax.rem(m, 2))

        z = lax.rem(2 * d + lax.div(e, 4) + 4 + swing(lax.div(n, 4)) + 8, 8)
        x = lax.rem(lax.rem(e, 4) + 2 + swing(lax.rem(n, 4)) + 4, 4)
        return lax.div(z, 2) * 8 + lax.rem(z, 2) * 4 + x

    bar = pltpu.get_barrier_semaphore()

    def greet_t(k):
        pl.semaphore_signal(bar, inc=1, device_id=at_t(lax.rem(t + k, 8)), device_id_type=MESH)

    def greet_p(k):
        pl.semaphore_signal(bar, inc=1, device_id=at_p(far_first(k)), device_id_type=MESH)

    loop(31, greet_p)
    loop(8, greet_t, 1)

    inputs = [
        pltpu.make_async_copy(src, dst, isem.at[n])
        for n, (src, dst) in enumerate(
            ((tok_hbm, tok), (og_hbm, og), (prob_hbm, prob), (id_hbm, ids), (slot_hbm, slots))
        )
    ]
    weights = [
        pltpu.make_async_copy(src, dst, wsem.at[n])
        for n, (src, dst) in enumerate(((wg_hbm, wg), (wu_hbm, wu), (wd_hbm, wd)))
    ]
    for c in inputs + weights:
        c.start()
    for c in inputs:
        c.wait()
    for dd in range(4):
        for q in range(8):
            at = slice(1024 * dd + 128 * q, 1024 * dd + 128 * q + 128)
            sendA[q, 0, :, 128 * dd : 128 * dd + 128] = tok[:, at]
            sendA[q, 1, :, 128 * dd : 128 * dd + 128] = og[:, at]
    slot, owner = slots[...], ids[...] * 8
    past = slot >= 16
    low = jnp.where(slot < 8, 64 + owner + slot, 120 + owner + slot)

    def places(extra):
        return jnp.where(slot < CAP, jnp.where(past, owner + slot - 16 + extra, low), -1)

    place_x, place_g, place_z = places(0), places(4), places(4 * lax.rem(e, 2))
    by_place = lax.broadcasted_iota(jnp.int32, (PLACES, 64), 0)
    tx = sum((by_place == place_x[k : k + 1]).astype(F32) for k in range(2)).astype(BF)
    t0, t1 = ((by_place == place_g[k : k + 1]).astype(BF) for k in range(2))
    by_token = lax.broadcasted_iota(jnp.int32, (64, PLACES), 1)
    tab[...] = sum((by_token == column(place_z[k : k + 1])).astype(F32) for k in range(2)).astype(BF)
    p0, p1 = (column(prob[k : k + 1]) for k in range(2))
    pl.semaphore_wait(bar, 38)

    def send_a(k):
        q = lax.rem(t + k, 8)
        remote(sendA.at[q], recvA.at[t], sA, rA, at_t(q)).start()

    loop(8, send_a, 1)
    recvA[t] = sendA[t]
    got(recvA.at[0:7], rA)

    rx = recvA[:, 0].astype(F32).reshape(64, 512).astype(BF)
    ry = recvA[:, 1].astype(F32).reshape(64, 512)
    xb = nn(tx, rx)
    gb = nn(t0, (p0 * ry).astype(BF)) + nn(t1, (p1 * ry).astype(BF))
    for dd in range(4):
        cols, to = slice(128 * dd, 128 * dd + 128), slice(8 * dd, 8 * dd + 8)
        sendR[to] = (xb[:64, cols] + gb[:64, cols]).reshape(8, 8, 128).astype(BF)
        for c in range(2):
            for a, v in enumerate((xb, gb)):
                sendC[c, to, a] = v[64 * c + 64 : 64 * c + 128, cols].reshape(8, 8, 128).astype(BF)

    def send_l(k):
        p = far_first(k)
        remote(sendR.at[p], recvR.at[b], sL, rL, at_p(p)).start()

    loop(31, send_l)
    pltpu.make_async_copy(sendR.at[b], recvR.at[b], rL).start()
    for c in range(2):
        sem = rC.at[c, lax.div(d, 2)]

        def send_c(k, c=c, sem=sem):
            p = far_first(k)
            remote(sendC.at[c, p], recvC.at[c, b], sC, sem, at_p(p)).start()

        loop(31, send_c)
        pltpu.make_async_copy(sendC.at[c, b], recvC.at[c, b], sem).start()

    def piece(src, a, i):
        return XG.at[src, a, pl.ds(8 * i, 8)]

    def send_d(i, a, src, dst, to_mate):
        ref = piece(src, a, i)
        remote(ref, ref, sD, rD.at[i, a, to_mate], at_t(dst)).start()

    def octet(c, p, a):
        return recvC[c, p, a].astype(F32)

    def start_d(i):
        for a in range(2):
            for k in (2, 1, 3):
                send_d(i, a, t, lax.rem(t + 2 * k, 8), 0)
            send_d(i, a, t, mate, 1)

    def relay_d(i, a):
        got(XG.at[0:3, a, pl.ds(8 * i, 8)], rD.at[i, a, 0])
        for k in (1, 3, 2):
            send_d(i, a, lax.rem(t + 2 * k, 8), mate, 1)

    def arrive_d(i, a):
        got(XG.at[0:4, a, pl.ds(8 * i, 8)], rD.at[i, a, 1])

    for c in weights:
        c.wait()

    def flip(src, dst):
        rows, cols = src.shape

        def one(r):
            at = pl.ds(pl.multiple_of(128 * r, 128), 128)
            for f in range(cols // 128):
                dst[128 * f : 128 * f + 128, at] = src[at, 128 * f : 128 * f + 128].T

        loop(rows // 128, one)

    flip(wd, wdT)
    got(recvR, rL)

    def rest(j):
        four = [recvR[4 * j + q].astype(F32) for q in range(4)]
        for a in range(2):
            XG[t, a, j] = jnp.concatenate([v[4 * a : 4 * a + 4] for v in four], axis=0).astype(BF)

    loop(8, rest)
    start_d(0)

    def prep(i):
        c, half = lax.div(i - 1, 2), lax.rem(i + 1, 2)
        got(recvC.at[c, pl.ds(16 * half, 16)], rC.at[c, half])

        def build(j):
            p = 16 * half + 2 * j
            for a in range(2):
                both = jnp.concatenate([octet(c, p, a), octet(c, p + 1, a)], axis=0)
                XG[t, a, 8 * i + j] = both.astype(BF)

        loop(8, build)
        start_d(i)

    def tile(i, owner, half):
        return 8 * i + 2 * owner + half

    def peer(dd):
        return (dd, e, t)

    UNITS = (slice(0, 2), slice(2, 3), slice(0, 3))

    def rs_send(i, m, w=2):
        u = UNITS[w]
        src, dst, dev = {
            0: (part.at[u, tile(i, opp, 0)], rs1.at[0, i, u], right),
            1: (part.at[u, tile(i, right, 1)], raw.at[0, i, u], right),
            2: (redS.at[0, i], red.at[0, i], right),
            3: (part.at[u, tile(i, opp, 1)], rs1.at[1, i, u], left),
            4: (part.at[u, tile(i, left, 0)], raw.at[1, i, u], left),
            5: (redS.at[1, i], red.at[1, i], left),
        }[m]
        sem = rR.at[i, {0: 0, 3: 1}.get(m, 2)]
        remote(src, dst, (sR1, sRaw, sRed)[m % 3], sem, peer(dev)).start()

    def rows_of(a, i):
        tiles = pl.ds(8 * i, 8)
        return jnp.concatenate([XG[q, a, tiles].reshape(128, 128) for q in range(8)], axis=1)

    def forward(i):
        tiles = pl.ds(8 * i, 8)
        relay_d(i, 0)
        arrive_d(i, 0)
        xs = rows_of(0, i)
        part[0, tiles] = nn(xs, wg[...]).astype(BF).reshape(8, 16, -1)
        part[1, tiles] = nn(xs, wu[...]).astype(BF).reshape(8, 16, -1)
        for m in (0, 3, 1, 4):
            rs_send(i, m, 0)
        relay_d(i, 1)
        arrive_d(i, 1)
        part[2, tiles] = nn(rows_of(1, i), wdT[...]).astype(BF).reshape(8, 16, -1)
        for m in (0, 3, 1, 4):
            rs_send(i, m, 1)

    def open_stage(i):
        @pl.when(i < S - 1)
        def _():
            prep(i + 1)

        forward(i)

    loop(S, open_stage)
    flip(wg, wgT)
    flip(wu, wuT)

    def middle(i):
        got(rs1.at[0, i], rR.at[i, 0])
        redS[0, i] = (part[:, tile(i, right, 0)].astype(F32) + rs1[0, i].astype(F32)).astype(BF)
        rs_send(i, 2)
        got(rs1.at[1, i], rR.at[i, 1])
        redS[1, i] = (part[:, tile(i, left, 1)].astype(F32) + rs1[1, i].astype(F32)).astype(BF)
        rs_send(i, 5)

    loop(S, middle)

    HID = (slice(0, 3), slice(3, 4), slice(4, 5))

    def ag_ref(i, owner, half=None):
        return H.at[1:3, i, pl.ds(2 * owner, 2) if half is None else 2 * owner + half]

    def hid_ref(n, owner, half=None):
        return H.at[0, HID[n], pl.ds(2 * owner, 2) if half is None else 2 * owner + half]

    def ring(ref, i, m, send, recv):
        src, dev = {
            0: (ref(i, d), right), 1: (ref(i, d), left),
            2: (ref(i, left, 0), right), 3: (ref(i, right, 1), left),
        }[m]
        remote(src, src, send, recv.at[i, min(m, 2)], peer(dev)).start()

    def ag_send(i, m):
        ring(ag_ref, i, m, sG, rG)

    def hid_send(n, m):
        ring(hid_ref, n, m, sN, rN)

    def own(i):
        got(raw.at[:, 0:2], rR.at[i, 2])
        for half, (ra, rb) in enumerate(((red, raw), (raw, red))):
            at, to = tile(i, d, half), 2 * d + half
            gate, up, grad = (
                part[u, at].astype(F32) + ra[0, i, u].astype(F32) + rb[1, i, u].astype(F32)
                for u in range(3)
            )
            s = jax.nn.sigmoid(gate)
            silu = gate * s
            H[0, i, to] = (silu * up).astype(BF)
            H[1, i, to] = (grad * up * s * (1.0 + gate * (1.0 - s))).astype(BF)
            H[2, i, to] = (grad * silu).astype(BF)
        ag_send(i, 0)
        ag_send(i, 1)

    def relay(i):
        for m, owner in enumerate((left, right)):
            got(ag_ref(i, owner), rG.at[i, m])
            ag_send(i, m + 2)

    def q_send(i, k):
        yy = lax.rem(y + k, 4)
        remote(qs.at[i, yy], recvQ.at[i, y], sQ, rQ.at[i], at_t(2 * yy + core)).start()

    def hid(u, i):
        return H[u, i].reshape(128, -1)

    def rows(i):
        got(H.at[1:3, i, 0:2], rG.at[i, 2])
        rg = nn(hid(1, i), wgT[...]) + nn(hid(2, i), wuT[...])
        for q in range(8):
            rgp[i, q % 2, q // 2] = rg[:, 128 * q : 128 * q + 128].astype(BF)
        remote(rgp.at[i, 1 - core], recvP.at[i], sP, rP.at[i], at_t(mate)).start()

    def pair(i):
        got(recvP.at[i], rP.at[i])
        qs[i] = (rgp[i, core].astype(F32) + recvP[i].astype(F32)).astype(BF)
        for k in (2, 1, 3):
            q_send(i, k)

    def back(i):
        tot = qs[i, y].astype(F32)
        got(recvQ.at[i, 0:3], rQ.at[i])
        for k in range(1, 4):
            tot = tot + recvQ[i, lax.rem(y + k, 4)].astype(F32)
        zs[i] = tot.reshape(16, 8, 128).astype(BF)

        @pl.when(i > 0)
        def _():
            c = lax.div(i + 1, 2)

            def put(o):
                p = 16 * lax.rem(i + 1, 2) + o

                @pl.when(p != b)
                def _():
                    remote(zs.at[i, o], recvZ.at[c, b], sZ, rZ, at_p(p)).start()

                @pl.when(p == b)
                def _():
                    pltpu.make_async_copy(zs.at[i, o], recvZ.at[c, b], rZ).start()

            loop(16, put)

        @pl.when(i == 0)
        def _():
            def put(k):
                p = far_first(k)
                remote(zs.at[0, lax.div(p, 2)], recvZ.at[0, b], sZ, rZ, at_p(p)).start()

            loop(31, put)
            pltpu.make_async_copy(zs.at[0, lax.div(b, 2)], recvZ.at[0, b], rZ).start()

    def turn(i):
        for q in range(8):
            v = XG[q, 0, pl.ds(8 * i, 8)].reshape(128, 128)
            XT[128 * q : 128 * q + 128, pl.ds(pl.multiple_of(128 * i, 128), 128)] = v.T

    def model_grad(u, out):
        out[0] = nn(XT[...], H[u].reshape(640, -1)).astype(BF)

    def down_part(lo, hi):
        g = jnp.concatenate(
            [XG[q, 1, 8 * lo : 8 * hi].reshape(128 * (hi - lo), 128) for q in range(8)], axis=1
        )
        return tn(H[0, lo:hi].reshape(128 * (hi - lo), -1), g)

    loop(S, turn)
    own(0)
    own(1)
    own(2)
    relay(0)
    relay(1)

    def cycle(i):
        @pl.when(i + 3 < S)
        def _():
            own(i + 3)

        @pl.when(i + 2 < S)
        def _():
            relay(i + 2)

        @pl.when(i == S - 3)
        def _():
            for n in (0, 1):
                for m in (0, 1):
                    hid_send(n, m)

        @pl.when(i >= 1)
        def _():
            pair(i - 1)

        @pl.when(i >= 2)
        def _():
            back(i - 2)

        rows(i)

    loop(S, cycle)
    pair(S - 1)
    back(S - 2)
    model_grad(1, gg_out)
    back(S - 1)
    for m in (0, 1):
        hid_send(2, m)

    def hid_relay(n):
        for m, owner in enumerate((left, right)):
            got(hid_ref(n, owner), rN.at[n, m])
            hid_send(n, m + 2)

    hid_relay(0)
    hid_relay(1)
    model_grad(2, gu_out)
    hid_relay(2)

    got(recvZ, rZ)
    for dd in range(4):
        z = recvZ[:, 8 * dd : 8 * dd + 8].astype(F32).reshape(PLACES, 128).astype(BF)
        part_rows = nn(tab[...], z).reshape(8, 8, 128).astype(BF)
        sendY[:, :, 128 * dd : 128 * dd + 128] = part_rows

    def y_send(k):
        q = lax.rem(t + k, 8)
        remote(sendY.at[q], recvY.at[t], sY, rY, at_t(q)).start()

    loop(8, y_send, 1)
    recvY[t] = sendY[t]
    for n in (0, 1):
        got(H.at[0, HID[n], 0:2], rN.at[n, 2])
    accd[...] = down_part(0, 4)

    for ref, sem in (
        (recvA.at[0:7], sA), (recvR.at[0:31], sL), (recvC.at[:, 0:31], sC), (XG.at[0:7], sD),
        (rs1, sR1), (raw, sRaw), (red, sRed), (H.at[1:3, :, 0:6], sG), (recvP, sP),
        (recvQ.at[:, 0:3], sQ), (recvZ.at[:, 0:31], sZ),
    ):
        sent(ref, sem)
    got(recvY.at[0:7], rY)
    for dd in range(4):
        for q in range(8):
            at = slice(1024 * dd + 128 * q, 1024 * dd + 128 * q + 128)
            y_out[:, at] = recvY[q, :, 128 * dd : 128 * dd + 128]
    got(H.at[0, HID[2], 0:2], rN.at[2, 2])
    gd_out[0] = (accd[...] + down_part(4, S)).astype(BF)
    sent(recvY.at[0:7], sY)
    sent(H.at[0, :, 0:6], sN)


def put_out(*refs):
    sems = refs[8]
    copies = [pltpu.make_async_copy(refs[n], refs[4 + n], sems.at[n]) for n in range(4)]
    for c in copies:
        c.start()
    for c in copies:
        c.wait()


def shards(tokens, out_grad, route_probs, expert_ids, slot_index, w_gate, w_up, w_down):
    wg, wu, wd = w_gate[0], w_up[0], w_down[0]
    dl, fl = wg.shape
    vm = pl.BlockSpec(memory_space=pltpu.VMEM)
    hbm = pl.BlockSpec(memory_space=pl.ANY)
    dma = pltpu.SemaphoreType.DMA

    def buf(*shape, dtype=BF):
        return pltpu.VMEM(shape, dtype)

    yv, gg, gu, gd = pl.pallas_call(
        kernel,
        name="expert_back",
        out_shape=(
            jax.ShapeDtypeStruct(tokens.shape, BF),
            jax.ShapeDtypeStruct(w_gate.shape, BF),
            jax.ShapeDtypeStruct(w_up.shape, BF),
            jax.ShapeDtypeStruct(w_down.shape, BF),
        ),
        in_specs=[hbm] * 8,
        out_specs=(vm, vm, vm, vm),
        scratch_shapes=[
            buf(8, 4096), buf(8, 4096), buf(2, 64, dtype=F32),
            buf(2, 64, dtype=jnp.int32), buf(2, 64, dtype=jnp.int32),
            buf(dl, fl), buf(dl, fl), buf(fl, dl), buf(fl, dl), buf(fl, dl), buf(dl, fl), buf(64, PLACES),
            buf(8, 2, 8, 512), buf(8, 2, 8, 512),
            buf(32, 8, 128), buf(32, 8, 128), buf(2, 32, 2, 8, 128), buf(2, 32, 2, 8, 128),
            buf(8, 2, 40, 16, 128), buf(dl, 640), buf(3, 40, 16, fl),
            buf(2, S, 3, 16, fl), buf(2, S, 3, 16, fl), buf(2, S, 3, 16, fl), buf(2, S, 3, 16, fl),
            buf(3, S, 8, 16, fl),
            buf(S, 2, 4, 128, 128), buf(S, 4, 128, 128), buf(S, 4, 128, 128), buf(S, 4, 128, 128),
            buf(S, 16, 8, 128), buf(3, 32, 8, 128), buf(8, 8, 512), buf(8, 8, 512),
            buf(fl, dl, dtype=F32),
            dma((5,)), dma((3,)), dma((17,)), dma((2, 2)), dma((S, 2, 2)),
            dma((S, 3)), dma((S, 3)), dma((3, 3)), dma((S,)), dma((S,)),
        ],
        compiler_params=pltpu.CompilerParams(
            collective_id=0, has_side_effects=True, vmem_limit_bytes=48 * 1024 * 1024
        ),
    )(*(
        pltpu.with_memory_space_constraint(v, pltpu.HBM)
        for v in (tokens, out_grad, route_probs.T, expert_ids.T, slot_index.T, wg, wu, wd)
    ))
    return pl.pallas_call(
        put_out,
        name="put_out",
        out_shape=tuple(jax.ShapeDtypeStruct(v.shape, v.dtype) for v in (yv, gg, gu, gd)),
        in_specs=[hbm] * 4,
        out_specs=(hbm,) * 4,
        scratch_shapes=[dma((4,))],
        compiler_params=pltpu.CompilerParams(vmem_limit_bytes=1024 * 1024),
    )(yv, gg, gu, gd)


def solution(mesh):
    placed = (
        P(("dp", "expert", "tensor"), None),
        P(("dp", "expert", "tensor"), None),
        P(("dp", "expert"), None),
        P(("dp", "expert"), None),
        P(("dp", "expert"), None),
        P("expert", "dp", "tensor"),
        P("expert", "dp", "tensor"),
        P("expert", "tensor", "dp"),
    )
    return jax.shard_map(
        shards,
        mesh=mesh,
        in_specs=placed,
        out_specs=(
            P(("dp", "expert", "tensor"), None),
            P("expert", "dp", "tensor"),
            P("expert", "dp", "tensor"),
            P("expert", "tensor", "dp"),
        ),
        check_vma=False,
    )
```

```python
import jax
import jax.numpy as jnp
from jax import lax
from jax.experimental import pallas as pl
from jax.experimental.pallas import tpu as pltpu
from jax.sharding import PartitionSpec as P

BF, F32 = jnp.bfloat16, jnp.float32
MESH = pl.DeviceIdType.MESH
S = 5
CAP = 20
PLACES = 192


def nt(a, b):
    return lax.dot_general(a, b, (((1,), (1,)), ((), ())), preferred_element_type=F32)


def tn(a, b):
    return lax.dot_general(a, b, (((0,), (0,)), ((), ())), preferred_element_type=F32)


def nn(a, b):
    return jnp.dot(a, b, preferred_element_type=F32)


def remote(src, dst, send, recv, dev):
    return pltpu.make_async_remote_copy(
        src_ref=src, dst_ref=dst, send_sem=send, recv_sem=recv, device_id=dev, device_id_type=MESH
    )


def loop(n, f, start=0):
    def step(i, c):
        f(i)
        return c

    lax.fori_loop(start, n, step, 0)


def column(row):
    n = row.shape[1]
    eye = lax.broadcasted_iota(jnp.int32, (n, n), 0) == lax.broadcasted_iota(jnp.int32, (n, n), 1)
    spread = jnp.where(eye, jnp.broadcast_to(row, (n, n)), jnp.zeros((n, n), row.dtype))
    return jnp.sum(spread, axis=1, keepdims=True)


def kernel(
    tok_hbm, og_hbm, prob_hbm, id_hbm, slot_hbm, wg_hbm, wu_hbm, wd_hbm,
    y_out, gg_out, gu_out, accd, h_last, g_last,
    tok, og, prob, ids, slots, wg, wu, wd, wgT, wuT, wdT, tab,
    sendA, recvA, sendR, recvR, sendC, XG, XT, part, rs1, raw, red, redS, H,
    rgp, recvP, qs, recvQ, zs, zr, recvZ, recvZr, sendY, recvY,
    isem, wsem, one, rA, rC, rD, rR, rG, rN, rP, rQ,
):
    d, e, t = lax.axis_index("dp"), lax.axis_index("expert"), lax.axis_index("tensor")
    b = d * 8 + e
    core, y = lax.rem(t, 2), lax.div(t, 2)
    mate = t + 1 - 2 * core
    right, left, opp = lax.rem(d + 1, 4), lax.rem(d + 3, 4), lax.rem(d + 2, 4)

    sA, sL, rL, sC, sD, sR1, sRaw, sRed, sG, sN, sP, sQ, sZ, rZ, sZr, rZr, sY, rY = (
        one.at[n] for n in range(18)
    )

    def at_t(tt):
        return (d, e, tt)

    def got(ref, sem):
        remote(ref, ref, sem, sem, (d, e, mate)).wait_recv()

    def sent(ref, sem):
        remote(ref, ref, sem, sem, (d, e, mate)).wait_send()

    def at_p(p):
        return (lax.div(p, 8), lax.rem(p, 8), t)

    def far_first(n):
        def swing(m):
            return lax.div(m + 1, 2) * (1 - 2 * lax.rem(m, 2))

        z = lax.rem(2 * d + lax.div(e, 4) + 4 + swing(lax.div(n, 4)) + 8, 8)
        x = lax.rem(lax.rem(e, 4) + 2 + swing(lax.rem(n, 4)) + 4, 4)
        return lax.div(z, 2) * 8 + lax.rem(z, 2) * 4 + x

    bar = pltpu.get_barrier_semaphore()

    def greet_t(k):
        pl.semaphore_signal(bar, inc=1, device_id=at_t(lax.rem(t + k, 8)), device_id_type=MESH)

    def greet_p(k):
        pl.semaphore_signal(bar, inc=1, device_id=at_p(far_first(k)), device_id_type=MESH)

    loop(31, greet_p)
    loop(8, greet_t, 1)

    inputs = [
        pltpu.make_async_copy(src, dst, isem.at[n])
        for n, (src, dst) in enumerate(
            ((tok_hbm, tok), (og_hbm, og), (prob_hbm, prob), (id_hbm, ids), (slot_hbm, slots))
        )
    ]
    weights = [
        pltpu.make_async_copy(src, dst, wsem.at[n])
        for n, (src, dst) in enumerate(((wg_hbm, wg), (wu_hbm, wu), (wd_hbm, wd)))
    ]
    for c in inputs + weights:
        c.start()
    for c in inputs:
        c.wait()
    for dd in range(4):
        for q in range(8):
            at = slice(1024 * dd + 128 * q, 1024 * dd + 128 * q + 128)
            sendA[0, q, :, 128 * dd : 128 * dd + 128] = tok[:, at]
            sendA[1, q, :, 128 * dd : 128 * dd + 128] = og[:, at]
    slot, owner = slots[...], ids[...] * 8
    past = slot >= 16
    low = 64 + 2 * owner + slot

    def places(extra):
        return jnp.where(slot < CAP, jnp.where(past, owner + slot - 16 + extra, low), -1)

    place_x, place_g, place_z = places(0), places(4), places(4 * lax.rem(e, 2))
    by_place = lax.broadcasted_iota(jnp.int32, (PLACES, 64), 0)
    tx = sum((by_place == place_x[k : k + 1]).astype(F32) for k in range(2)).astype(BF)
    t0, t1 = ((by_place == place_g[k : k + 1]).astype(BF) for k in range(2))
    by_token = lax.broadcasted_iota(jnp.int32, (64, PLACES), 1)
    tab[...] = sum((by_token == column(place_z[k : k + 1])).astype(F32) for k in range(2)).astype(BF)
    p0, p1 = (column(prob[k : k + 1]) for k in range(2))
    for c in weights:
        c.wait()

    def flip(src, dst):
        rows, cols = src.shape

        def one(r):
            at = pl.ds(pl.multiple_of(128 * r, 128), 128)
            for f in range(cols // 128):
                dst[128 * f : 128 * f + 128, at] = src[at, 128 * f : 128 * f + 128].T

        loop(rows // 128, one)

    flip(wd, wdT)
    pl.semaphore_wait(bar, 38)

    for a in range(2):
        def send_a(k, a=a):
            q = lax.rem(t + k, 8)
            remote(sendA.at[a, q], recvA.at[a, t], sA, rA.at[a], at_t(q)).start()

        loop(8, send_a, 1)
        recvA[a, t] = sendA[a, t]

    got(recvA.at[0, 0:7], rA.at[0])
    rx = recvA[0].astype(F32).reshape(64, 512).astype(BF)

    z0, x0 = 2 * d + lax.div(e, 4), lax.rem(e, 4)
    FAR = (4, 3, 5, 2, 6, 1, 7, 0)

    def device_at(dz, dx):
        z = lax.rem(z0 + dz, 8)
        return lax.div(z, 2), 4 * lax.rem(z, 2) + lax.rem(x0 + dx, 4)

    def send_stage(delta, a):
        i, dx = delta + delta // 2, (4 - delta) % 4
        for dz in FAR:
            pd, pe = device_at(dz, dx)
            src, dst = sendC.at[a, 8 * pd + pe], XG.at[t, a, 8 * i + z0]
            if dz or dx:
                remote(src, dst, sC, rC.at[i, a], (pd, pe, t)).start()
            else:
                pltpu.make_async_copy(src, dst, rC.at[i, a]).start()

    def put_slots(a, v):
        for dd in range(4):
            cols = slice(128 * dd, 128 * dd + 128)
            sendC[a, 8 * dd : 8 * dd + 8] = v[:, cols].reshape(8, 16, 128).astype(BF)

    put_slots(0, nn(tx[64:], rx))
    send_stage(0, 0)
    got(recvA.at[1, 0:7], rA.at[1])
    ry = recvA[1].astype(F32).reshape(64, 512)
    s0, s1 = (p0 * ry).astype(BF), (p1 * ry).astype(BF)
    put_slots(1, nn(t0[64:], s0) + nn(t1[64:], s1))
    send_stage(0, 1)
    for a in range(2):
        send_stage(1, a)
    xb, gb = nn(tx[:64], rx), nn(t0[:64], s0) + nn(t1[:64], s1)
    for dd in range(4):
        cols = slice(128 * dd, 128 * dd + 128)
        sendR[8 * dd : 8 * dd + 8] = (xb[:, cols] + gb[:, cols]).reshape(8, 8, 128).astype(BF)

    def send_l(k):
        p = far_first(k)
        remote(sendR.at[p], recvR.at[b], sL, rL, at_p(p)).start()

    loop(31, send_l)
    pltpu.make_async_copy(sendR.at[b], recvR.at[b], rL).start()
    for delta in (2, 3):
        for a in range(2):
            send_stage(delta, a)

    def piece(src, a, i):
        return XG.at[src, a, pl.ds(8 * i, 8)]

    def send_d(i, a, src, dst, to_mate):
        ref = piece(src, a, i)
        remote(ref, ref, sD, rD.at[i, a, to_mate], at_t(dst)).start()

    def start_d(i, a):
        for k in (2, 1, 3):
            send_d(i, a, t, lax.rem(t + 2 * k, 8), 0)
        send_d(i, a, t, mate, 1)

    def relay_d(i, a):
        got(XG.at[0:3, a, pl.ds(8 * i, 8)], rD.at[i, a, 0])
        for k in (1, 3, 2):
            send_d(i, a, lax.rem(t + 2 * k, 8), mate, 1)

    def arrive_d(i, a):
        got(XG.at[0:4, a, pl.ds(8 * i, 8)], rD.at[i, a, 1])

    def rest(j):
        four = [recvR[4 * j + q].astype(F32) for q in range(4)]
        for a in range(2):
            XG[t, a, 16 + j] = jnp.concatenate([v[4 * a : 4 * a + 4] for v in four], axis=0).astype(BF)

    def prep(i):
        @pl.when(i == 2)
        def _():
            got(recvR, rL)
            loop(8, rest)

        for a in range(2):
            @pl.when(i != 2)
            def _(a=a):
                got(XG.at[t, a, pl.ds(8 * i, 8)], rC.at[i, a])

            start_d(i, a)

    prep(0)

    def tile(i, owner, half):
        return 8 * i + 2 * owner + half

    def peer(dd):
        return (dd, e, t)

    UNITS = (slice(0, 1), slice(1, 2), slice(2, 3), slice(0, 3))

    def rs_send(i, m, w=3):
        u = UNITS[w]
        src, dst, dev = {
            0: (part.at[u, tile(i, opp, 0)], rs1.at[0, i, u], right),
            1: (part.at[u, tile(i, right, 1)], raw.at[0, i, u], right),
            2: (redS.at[0, i], red.at[0, i], right),
            3: (part.at[u, tile(i, opp, 1)], rs1.at[1, i, u], left),
            4: (part.at[u, tile(i, left, 0)], raw.at[1, i, u], left),
            5: (redS.at[1, i], red.at[1, i], left),
        }[m]
        sem = rR.at[i, {0: 0, 3: 1}.get(m, 2)]
        remote(src, dst, (sR1, sRaw, sRed)[m % 3], sem, peer(dev)).start()

    def rows_of(a, i):
        tiles = pl.ds(8 * i, 8)
        return jnp.concatenate([XG[q, a, tiles].reshape(128, 128) for q in range(8)], axis=1)

    def forward(i):
        tiles = pl.ds(8 * i, 8)
        relay_d(i, 0)
        arrive_d(i, 0)
        xs = rows_of(0, i)
        for w, wt in enumerate((wg, wu)):
            part[w, tiles] = nn(xs, wt[...]).astype(BF).reshape(8, 16, -1)
            for m in (0, 3, 1, 4):
                rs_send(i, m, w)
        relay_d(i, 1)
        arrive_d(i, 1)
        part[2, tiles] = nn(rows_of(1, i), wdT[...]).astype(BF).reshape(8, 16, -1)
        for m in (0, 3, 1, 4):
            rs_send(i, m, 2)

    def open_stage(i):
        @pl.when(i < S - 1)
        def _():
            prep(i + 1)

        forward(i)

    loop(S, open_stage)
    flip(wg, wgT)
    flip(wu, wuT)

    def middle(i):
        got(rs1.at[0, i], rR.at[i, 0])
        redS[0, i] = (part[:, tile(i, right, 0)].astype(F32) + rs1[0, i].astype(F32)).astype(BF)
        rs_send(i, 2)
        got(rs1.at[1, i], rR.at[i, 1])
        redS[1, i] = (part[:, tile(i, left, 1)].astype(F32) + rs1[1, i].astype(F32)).astype(BF)
        rs_send(i, 5)

    loop(S, middle)

    HID = (slice(0, 3), slice(3, 4), slice(4, 5))

    def ag_ref(i, owner, half=None):
        return H.at[1:3, i, pl.ds(2 * owner, 2) if half is None else 2 * owner + half]

    def hid_ref(n, owner, half=None):
        return H.at[0, HID[n], pl.ds(2 * owner, 2) if half is None else 2 * owner + half]

    def ring(ref, i, m, send, recv):
        src, dev = {
            0: (ref(i, d), right), 1: (ref(i, d), left),
            2: (ref(i, left, 0), right), 3: (ref(i, right, 1), left),
        }[m]
        remote(src, src, send, recv.at[i, min(m, 2)], peer(dev)).start()

    def ag_send(i, m):
        ring(ag_ref, i, m, sG, rG)

    def hid_send(n, m):
        ring(hid_ref, n, m, sN, rN)

    def own(i):
        got(raw.at[:, 0:2], rR.at[i, 2])
        for half, (ra, rb) in enumerate(((red, raw), (raw, red))):
            at, to = tile(i, d, half), 2 * d + half
            gate, up, grad = (
                part[u, at].astype(F32) + ra[0, i, u].astype(F32) + rb[1, i, u].astype(F32)
                for u in range(3)
            )
            s = jax.nn.sigmoid(gate)
            silu = gate * s
            H[0, i, to] = (silu * up).astype(BF)
            H[1, i, to] = (grad * up * s * (1.0 + gate * (1.0 - s))).astype(BF)
            H[2, i, to] = (grad * silu).astype(BF)
        ag_send(i, 0)
        ag_send(i, 1)

    def relay(i):
        for m, owner in enumerate((left, right)):
            got(ag_ref(i, owner), rG.at[i, m])
            ag_send(i, m + 2)

    def q_send(i, k):
        yy = lax.rem(y + k, 4)
        remote(qs.at[i, yy], recvQ.at[i, y], sQ, rQ.at[i], at_t(2 * yy + core)).start()

    def hid(u, i):
        return H[u, i].reshape(128, -1)

    def rows(i):
        got(H.at[1:3, i, 0:2], rG.at[i, 2])
        rg = nn(hid(1, i), wgT[...]) + nn(hid(2, i), wuT[...])
        for q in range(8):
            rgp[i, q % 2, q // 2] = rg[:, 128 * q : 128 * q + 128].astype(BF)
        remote(rgp.at[i, 1 - core], recvP.at[i], sP, rP.at[i], at_t(mate)).start()

    def pair(i):
        got(recvP.at[i], rP.at[i])
        qs[i] = (rgp[i, core].astype(F32) + recvP[i].astype(F32)).astype(BF)
        for k in (2, 1, 3):
            q_send(i, k)

    def back(i):
        tot = qs[i, y].astype(F32)
        got(recvQ.at[i, 0:3], rQ.at[i])
        for k in range(1, 4):
            tot = tot + recvQ[i, lax.rem(y + k, 4)].astype(F32)
        @pl.when(i != 2)
        def _():
            zs[i] = tot.reshape(8, 16, 128).astype(BF)
            x = lax.rem(x0 + i - lax.div(i, 3), 4)
            for dz in FAR:
                z = lax.rem(z0 + dz, 8)
                pd, pe = lax.div(z, 2), 4 * lax.rem(z, 2) + x
                if dz:
                    remote(zs.at[i, z], recvZ.at[b], sZ, rZ, (pd, pe, t)).start()
                else:
                    @pl.when(i != 0)
                    def _():
                        remote(zs.at[i, z], recvZ.at[b], sZ, rZ, (pd, pe, t)).start()

                    @pl.when(i == 0)
                    def _():
                        pltpu.make_async_copy(zs.at[i, z], recvZ.at[b], rZ).start()

        @pl.when(i == 2)
        def _():
            zr[...] = tot.reshape(16, 8, 128).astype(BF)

            def put(k):
                p = far_first(k)
                remote(zr.at[lax.div(p, 2)], recvZr.at[b], sZr, rZr, at_p(p)).start()

            loop(31, put)
            pltpu.make_async_copy(zr.at[lax.div(b, 2)], recvZr.at[b], rZr).start()

    def turn(i):
        for q in range(8):
            v = XG[q, 0, pl.ds(8 * i, 8)].reshape(128, 128)
            XT[128 * q : 128 * q + 128, pl.ds(pl.multiple_of(128 * i, 128), 128)] = v.T

    def model_grad(u, out):
        out[0] = nn(XT[...], H[u].reshape(640, -1)).astype(BF)

    def down_part(lo, hi):
        g = jnp.concatenate(
            [XG[q, 1, 8 * lo : 8 * hi].reshape(128 * (hi - lo), 128) for q in range(8)], axis=1
        )
        return tn(H[0, lo:hi].reshape(128 * (hi - lo), -1), g)

    loop(S, turn)
    own(0)
    own(1)
    own(2)
    relay(0)
    relay(1)

    def cycle(i):
        @pl.when(i + 3 < S)
        def _():
            own(i + 3)

        @pl.when(i + 2 < S)
        def _():
            relay(i + 2)

        @pl.when(i == S - 3)
        def _():
            for n in (0, 1):
                for m in (0, 1):
                    hid_send(n, m)

        @pl.when(i >= 1)
        def _():
            pair(i - 1)

        @pl.when(i >= 2)
        def _():
            back(i - 2)

        rows(i)

    loop(S, cycle)
    def hid_relay(n):
        for m, owner in enumerate((left, right)):
            got(hid_ref(n, owner), rN.at[n, m])
            hid_send(n, m + 2)

    pair(S - 1)
    back(S - 2)
    model_grad(1, gg_out)
    back(S - 1)
    for m in (0, 1):
        hid_send(2, m)
    hid_relay(0)
    hid_relay(1)
    hid_relay(2)

    got(recvZ, rZ)
    got(recvZr, rZr)
    for dd in range(4):
        at = slice(8 * dd, 8 * dd + 8)
        past16 = recvZr[at].astype(F32).reshape(64, 128).astype(BF)
        z = jnp.concatenate([past16, recvZ[at].reshape(128, 128)], axis=0)
        part_rows = nn(tab[...], z).reshape(8, 8, 128).astype(BF)
        sendY[:, :, 128 * dd : 128 * dd + 128] = part_rows

    def y_send(k):
        q = lax.rem(t + k, 8)
        remote(sendY.at[q], recvY.at[t], sY, rY, at_t(q)).start()

    loop(8, y_send, 1)
    recvY[t] = sendY[t]
    model_grad(2, gu_out)
    for n in (0, 1):
        got(H.at[0, HID[n], 0:2], rN.at[n, 2])
    accd[...] = down_part(0, 4)
    g_last[...] = rows_of(1, 4)

    for ref, sem in (
        (recvA.at[:, 0:7], sA), (recvR.at[0:31], sL), (sendC.at[:, 0:31], sC), (XG.at[0:7], sD),
        (rs1, sR1), (raw, sRaw), (red, sRed), (H.at[1:3, :, 0:6], sG), (recvP, sP),
        (recvQ.at[:, 0:3], sQ), (recvZ.at[0:31], sZ), (recvZr.at[0:31], sZr),
    ):
        sent(ref, sem)
    got(recvY.at[0:7], rY)
    for dd in range(4):
        for q in range(8):
            at = slice(1024 * dd + 128 * q, 1024 * dd + 128 * q + 128)
            y_out[:, at] = recvY[q, :, 128 * dd : 128 * dd + 128]
    got(H.at[0, HID[2], 0:2], rN.at[2, 2])
    h_last[...] = H[0, 4].reshape(128, -1)
    sent(recvY.at[0:7], sY)
    sent(H.at[0, :, 0:6], sN)


def put_out(yv, gg, gu, accd, h_last, g_last, y_out, gg_out, gu_out, gd_out, gd, sems):
    copies = [
        pltpu.make_async_copy(src, dst, sems.at[n])
        for n, (src, dst) in enumerate(((gg, gg_out), (gu, gu_out), (yv, y_out), (gd, gd_out)))
    ]
    for c in copies[:3]:
        c.start()
    gd[0] = (accd[...] + tn(h_last[...], g_last[...])).astype(BF)
    copies[3].start()
    for c in copies:
        c.wait()


def shards(tokens, out_grad, route_probs, expert_ids, slot_index, w_gate, w_up, w_down):
    wg, wu, wd = w_gate[0], w_up[0], w_down[0]
    dl, fl = wg.shape
    vm = pl.BlockSpec(memory_space=pltpu.VMEM)
    hbm = pl.BlockSpec(memory_space=pl.ANY)
    dma = pltpu.SemaphoreType.DMA

    def buf(*shape, dtype=BF):
        return pltpu.VMEM(shape, dtype)

    parts = pl.pallas_call(
        kernel,
        name="expert_back",
        out_shape=(
            jax.ShapeDtypeStruct(tokens.shape, BF),
            jax.ShapeDtypeStruct(w_gate.shape, BF),
            jax.ShapeDtypeStruct(w_up.shape, BF),
            jax.ShapeDtypeStruct((fl, dl), F32),
            jax.ShapeDtypeStruct((128, fl), BF),
            jax.ShapeDtypeStruct((128, dl), BF),
        ),
        in_specs=[hbm] * 8,
        out_specs=(vm,) * 6,
        scratch_shapes=[
            buf(8, 4096), buf(8, 4096), buf(2, 64, dtype=F32),
            buf(2, 64, dtype=jnp.int32), buf(2, 64, dtype=jnp.int32),
            buf(dl, fl), buf(dl, fl), buf(fl, dl), buf(fl, dl), buf(fl, dl), buf(dl, fl), buf(64, PLACES),
            buf(2, 8, 8, 512), buf(2, 8, 8, 512),
            buf(32, 8, 128), buf(32, 8, 128), buf(2, 32, 16, 128),
            buf(8, 2, 40, 16, 128), buf(dl, 640), buf(3, 40, 16, fl),
            buf(2, S, 3, 16, fl), buf(2, S, 3, 16, fl), buf(2, S, 3, 16, fl), buf(2, S, 3, 16, fl),
            buf(3, S, 8, 16, fl),
            buf(S, 2, 4, 128, 128), buf(S, 4, 128, 128), buf(S, 4, 128, 128), buf(S, 4, 128, 128),
            buf(S, 8, 16, 128), buf(16, 8, 128), buf(32, 16, 128), buf(32, 8, 128), buf(8, 8, 512), buf(8, 8, 512),
            dma((5,)), dma((3,)), dma((18,)), dma((2,)), dma((S, 2)), dma((S, 2, 2)),
            dma((S, 3)), dma((S, 3)), dma((3, 3)), dma((S,)), dma((S,)),
        ],
        compiler_params=pltpu.CompilerParams(
            collective_id=0, has_side_effects=True, vmem_limit_bytes=46 * 1024 * 1024
        ),
    )(*(
        pltpu.with_memory_space_constraint(v, pltpu.HBM)
        for v in (tokens, out_grad, route_probs.T, expert_ids.T, slot_index.T, wg, wu, wd)
    ))
    return pl.pallas_call(
        put_out,
        name="put_out",
        out_shape=tuple(
            jax.ShapeDtypeStruct(v.shape, BF) for v in (tokens, w_gate, w_up, w_down)
        ),
        in_specs=[vm] * 6,
        out_specs=(hbm,) * 4,
        scratch_shapes=[buf(*w_down.shape), dma((4,))],
        compiler_params=pltpu.CompilerParams(vmem_limit_bytes=16 * 1024 * 1024),
    )(*parts)


def solution(mesh):
    placed = (
        P(("dp", "expert", "tensor"), None),
        P(("dp", "expert", "tensor"), None),
        P(("dp", "expert"), None),
        P(("dp", "expert"), None),
        P(("dp", "expert"), None),
        P("expert", "dp", "tensor"),
        P("expert", "dp", "tensor"),
        P("expert", "tensor", "dp"),
    )
    return jax.shard_map(
        shards,
        mesh=mesh,
        in_specs=placed,
        out_specs=(
            P(("dp", "expert", "tensor"), None),
            P("expert", "dp", "tensor"),
            P("expert", "dp", "tensor"),
            P("expert", "tensor", "dp"),
        ),
        check_vma=False,
    )
```

```python
import jax
import jax.numpy as jnp
from jax import lax
from jax.experimental import pallas as pl
from jax.experimental.pallas import tpu as pltpu
from jax.sharding import PartitionSpec as P

BF, F32 = jnp.bfloat16, jnp.float32
MESH = pl.DeviceIdType.MESH
S = 5
CAP = 20
PLACES = 192


def nt(a, b):
    return lax.dot_general(a, b, (((1,), (1,)), ((), ())), preferred_element_type=F32)


def tn(a, b):
    return lax.dot_general(a, b, (((0,), (0,)), ((), ())), preferred_element_type=F32)


def nn(a, b):
    return jnp.dot(a, b, preferred_element_type=F32)


def remote(src, dst, send, recv, dev):
    return pltpu.make_async_remote_copy(
        src_ref=src, dst_ref=dst, send_sem=send, recv_sem=recv, device_id=dev, device_id_type=MESH
    )


def loop(n, f, start=0):
    def step(i, c):
        f(i)
        return c

    lax.fori_loop(start, n, step, 0)


def column(row):
    n = row.shape[1]
    eye = lax.broadcasted_iota(jnp.int32, (n, n), 0) == lax.broadcasted_iota(jnp.int32, (n, n), 1)
    spread = jnp.where(eye, jnp.broadcast_to(row, (n, n)), jnp.zeros((n, n), row.dtype))
    return jnp.sum(spread, axis=1, keepdims=True)


def kernel(
    tok_hbm, og_hbm, prob_hbm, id_hbm, slot_hbm, wg_hbm, wu_hbm, wd_hbm,
    y_out, gg_out, gu_out, accd, h_last, g_last,
    tok, og, prob, ids, slots, wg, wu, wd, wgT, wuT, wdT, tab,
    sendA, recvA, sendR, recvR, sendC, XG, XT, part, rs1, raw, red, redS, H,
    rgp, recvP, qs, recvQ, zs, zr, recvZ, recvZr, sendY, recvY,
    isem, wsem, one, rA, rC, rD, rR, rG, rN, rP, rQ,
):
    d, e, t = lax.axis_index("dp"), lax.axis_index("expert"), lax.axis_index("tensor")
    b = d * 8 + e
    core, y = lax.rem(t, 2), lax.div(t, 2)
    mate = t + 1 - 2 * core
    right, left, opp = lax.rem(d + 1, 4), lax.rem(d + 3, 4), lax.rem(d + 2, 4)

    sA, sL, rL, sC, sD, sR1, sRaw, sRed, sG, sN, sP, sQ, sZ, rZ, sZr, rZr, sY, rY = (
        one.at[n] for n in range(18)
    )

    def at_t(tt):
        return (d, e, tt)

    def got(ref, sem):
        remote(ref, ref, sem, sem, (d, e, mate)).wait_recv()

    def sent(ref, sem):
        remote(ref, ref, sem, sem, (d, e, mate)).wait_send()

    def at_p(p):
        return (lax.div(p, 8), lax.rem(p, 8), t)

    def far_first(n):
        def swing(m):
            return lax.div(m + 1, 2) * (1 - 2 * lax.rem(m, 2))

        z = lax.rem(2 * d + lax.div(e, 4) + 4 + swing(lax.div(n, 4)) + 8, 8)
        x = lax.rem(lax.rem(e, 4) + 2 + swing(lax.rem(n, 4)) + 4, 4)
        return lax.div(z, 2) * 8 + lax.rem(z, 2) * 4 + x

    bar = pltpu.get_barrier_semaphore()

    def greet_t(k):
        pl.semaphore_signal(bar, inc=1, device_id=at_t(lax.rem(t + k, 8)), device_id_type=MESH)

    def greet_p(k):
        pl.semaphore_signal(bar, inc=1, device_id=at_p(far_first(k)), device_id_type=MESH)

    loop(31, greet_p)
    loop(8, greet_t, 1)

    inputs = [
        pltpu.make_async_copy(src, dst, isem.at[n])
        for n, (src, dst) in enumerate(
            ((tok_hbm, tok), (og_hbm, og), (prob_hbm, prob), (id_hbm, ids), (slot_hbm, slots))
        )
    ]
    weights = [
        pltpu.make_async_copy(src, dst, wsem.at[n])
        for n, (src, dst) in enumerate(((wg_hbm, wg), (wu_hbm, wu), (wd_hbm, wd)))
    ]
    for c in inputs + weights:
        c.start()
    for c in inputs:
        c.wait()
    for dd in range(4):
        for q in range(8):
            at = slice(1024 * dd + 128 * q, 1024 * dd + 128 * q + 128)
            sendA[0, q, :, 128 * dd : 128 * dd + 128] = tok[:, at]
            sendA[1, q, :, 128 * dd : 128 * dd + 128] = og[:, at]
    slot, owner = slots[...], ids[...] * 8
    past = slot >= 16
    low = 64 + 2 * owner + slot

    def places(extra):
        return jnp.where(slot < CAP, jnp.where(past, owner + slot - 16 + extra, low), -1)

    place_x, place_g, place_z = places(0), places(4), places(4 * lax.rem(e, 2))
    by_place = lax.broadcasted_iota(jnp.int32, (PLACES, 64), 0)
    tx = sum((by_place == place_x[k : k + 1]).astype(F32) for k in range(2)).astype(BF)
    t0, t1 = ((by_place == place_g[k : k + 1]).astype(BF) for k in range(2))
    by_token = lax.broadcasted_iota(jnp.int32, (64, PLACES), 1)
    tab[...] = sum((by_token == column(place_z[k : k + 1])).astype(F32) for k in range(2)).astype(BF)
    p0, p1 = (column(prob[k : k + 1]) for k in range(2))
    for c in weights:
        c.wait()

    def flip(src, dst):
        rows, cols = src.shape

        def one(r):
            at = pl.ds(pl.multiple_of(128 * r, 128), 128)
            for f in range(cols // 128):
                dst[128 * f : 128 * f + 128, at] = src[at, 128 * f : 128 * f + 128].T

        loop(rows // 128, one)

    flip(wd, wdT)
    pl.semaphore_wait(bar, 38)

    for a in range(2):
        def send_a(k, a=a):
            q = lax.rem(t + k, 8)
            remote(sendA.at[a, q], recvA.at[a, t], sA, rA.at[a], at_t(q)).start()

        for k in (4, 3, 5, 2, 6, 1, 7):
            send_a(k)
        recvA[a, t] = sendA[a, t]

    got(recvA.at[0, 0:7], rA.at[0])
    rx = recvA[0].astype(F32).reshape(64, 512).astype(BF)

    z0, x0 = 2 * d + lax.div(e, 4), lax.rem(e, 4)
    FAR = (4, 3, 5, 2, 6, 1, 7, 0)

    def device_at(dz, dx):
        z = lax.rem(z0 + dz, 8)
        return lax.div(z, 2), 4 * lax.rem(z, 2) + lax.rem(x0 + dx, 4)

    def send_stage(delta, a):
        step = (delta + 3) % 4
        i, dx = step + step // 2, (4 - delta) % 4
        for dz in FAR:
            pd, pe = device_at(dz, dx)
            src, dst = sendC.at[a, 8 * pd + pe], XG.at[t, a, 8 * i + z0]
            if dz or dx:
                remote(src, dst, sC, rC.at[i, a], (pd, pe, t)).start()
            else:
                pltpu.make_async_copy(src, dst, rC.at[i, a]).start()

    def put_slots(a, v):
        for dd in range(4):
            cols = slice(128 * dd, 128 * dd + 128)
            sendC[a, 8 * dd : 8 * dd + 8] = v[:, cols].reshape(8, 16, 128).astype(BF)

    put_slots(0, nn(tx[64:], rx))
    send_stage(1, 0)
    got(recvA.at[1, 0:7], rA.at[1])
    ry = recvA[1].astype(F32).reshape(64, 512)
    s0, s1 = (p0 * ry).astype(BF), (p1 * ry).astype(BF)
    put_slots(1, nn(t0[64:], s0) + nn(t1[64:], s1))
    send_stage(1, 1)
    for a in range(2):
        send_stage(2, a)
    xb, gb = nn(tx[:64], rx), nn(t0[:64], s0) + nn(t1[:64], s1)
    for dd in range(4):
        cols = slice(128 * dd, 128 * dd + 128)
        sendR[8 * dd : 8 * dd + 8] = (xb[:, cols] + gb[:, cols]).reshape(8, 8, 128).astype(BF)

    def send_l(k):
        p = far_first(k)
        remote(sendR.at[p], recvR.at[b], sL, rL, at_p(p)).start()

    loop(31, send_l)
    pltpu.make_async_copy(sendR.at[b], recvR.at[b], rL).start()
    for delta in (3, 0):
        for a in range(2):
            send_stage(delta, a)

    def piece(src, a, i):
        return XG.at[src, a, pl.ds(8 * i, 8)]

    def send_d(i, a, src, dst, to_mate):
        ref = piece(src, a, i)
        remote(ref, ref, sD, rD.at[i, a, to_mate], at_t(dst)).start()

    def start_d(i, a):
        for k in (2, 1, 3):
            send_d(i, a, t, lax.rem(t + 2 * k, 8), 0)
        send_d(i, a, t, mate, 1)

    def relay_d(i, a):
        got(XG.at[0:3, a, pl.ds(8 * i, 8)], rD.at[i, a, 0])
        for k in (1, 3, 2):
            send_d(i, a, lax.rem(t + 2 * k, 8), mate, 1)

    def arrive_d(i, a):
        got(XG.at[0:4, a, pl.ds(8 * i, 8)], rD.at[i, a, 1])

    def rest(j):
        four = [recvR[4 * j + q].astype(F32) for q in range(4)]
        for a in range(2):
            XG[t, a, 16 + j] = jnp.concatenate([v[4 * a : 4 * a + 4] for v in four], axis=0).astype(BF)

    def prep(i):
        @pl.when(i == 2)
        def _():
            got(recvR, rL)
            loop(8, rest)

        for a in range(2):
            @pl.when(i != 2)
            def _(a=a):
                got(XG.at[t, a, pl.ds(8 * i, 8)], rC.at[i, a])

            start_d(i, a)

    prep(0)

    def tile(i, owner, half):
        return 8 * i + 2 * owner + half

    def peer(dd):
        return (dd, e, t)

    UNITS = (slice(0, 1), slice(1, 2), slice(2, 3), slice(0, 3))

    def rs_send(i, m, w=3):
        u = UNITS[w]
        src, dst, dev = {
            0: (part.at[u, tile(i, opp, 0)], rs1.at[0, i, u], right),
            1: (part.at[u, tile(i, right, 1)], raw.at[0, i, u], right),
            2: (redS.at[0, i], red.at[0, i], right),
            3: (part.at[u, tile(i, opp, 1)], rs1.at[1, i, u], left),
            4: (part.at[u, tile(i, left, 0)], raw.at[1, i, u], left),
            5: (redS.at[1, i], red.at[1, i], left),
        }[m]
        sem = rR.at[i, {0: 0, 3: 1}.get(m, 2)]
        remote(src, dst, (sR1, sRaw, sRed)[m % 3], sem, peer(dev)).start()

    def rows_of(a, i):
        tiles = pl.ds(8 * i, 8)
        return jnp.concatenate([XG[q, a, tiles].reshape(128, 128) for q in range(8)], axis=1)

    def forward(i):
        tiles = pl.ds(8 * i, 8)
        relay_d(i, 0)
        arrive_d(i, 0)
        xs = rows_of(0, i)
        for w, wt in enumerate((wg, wu)):
            part[w, tiles] = nn(xs, wt[...]).astype(BF).reshape(8, 16, -1)
            for m in (0, 3, 1, 4):
                rs_send(i, m, w)
        relay_d(i, 1)
        arrive_d(i, 1)
        part[2, tiles] = nn(rows_of(1, i), wdT[...]).astype(BF).reshape(8, 16, -1)
        for m in (0, 3, 1, 4):
            rs_send(i, m, 2)

    def open_stage(i):
        @pl.when(i < S - 1)
        def _():
            prep(i + 1)

        forward(i)

    loop(S, open_stage)
    flip(wg, wgT)
    flip(wu, wuT)

    def middle(i):
        got(rs1.at[0, i], rR.at[i, 0])
        redS[0, i] = (part[:, tile(i, right, 0)].astype(F32) + rs1[0, i].astype(F32)).astype(BF)
        rs_send(i, 2)
        got(rs1.at[1, i], rR.at[i, 1])
        redS[1, i] = (part[:, tile(i, left, 1)].astype(F32) + rs1[1, i].astype(F32)).astype(BF)
        rs_send(i, 5)

    loop(S, middle)

    HID = (slice(0, 3), slice(3, 4), slice(4, 5))

    def ag_ref(i, owner, half=None):
        return H.at[1:3, i, pl.ds(2 * owner, 2) if half is None else 2 * owner + half]

    def hid_ref(n, owner, half=None):
        return H.at[0, HID[n], pl.ds(2 * owner, 2) if half is None else 2 * owner + half]

    def ring(ref, i, m, send, recv):
        src, dev = {
            0: (ref(i, d), right), 1: (ref(i, d), left),
            2: (ref(i, left, 0), right), 3: (ref(i, right, 1), left),
        }[m]
        remote(src, src, send, recv.at[i, min(m, 2)], peer(dev)).start()

    def ag_send(i, m):
        ring(ag_ref, i, m, sG, rG)

    def hid_send(n, m):
        ring(hid_ref, n, m, sN, rN)

    def own(i):
        got(raw.at[:, 0:2], rR.at[i, 2])
        for half, (ra, rb) in enumerate(((red, raw), (raw, red))):
            at, to = tile(i, d, half), 2 * d + half
            gate, up, grad = (
                part[u, at].astype(F32) + ra[0, i, u].astype(F32) + rb[1, i, u].astype(F32)
                for u in range(3)
            )
            s = jax.nn.sigmoid(gate)
            silu = gate * s
            H[0, i, to] = (silu * up).astype(BF)
            H[1, i, to] = (grad * up * s * (1.0 + gate * (1.0 - s))).astype(BF)
            H[2, i, to] = (grad * silu).astype(BF)
        ag_send(i, 0)
        ag_send(i, 1)

    def relay(i):
        for m, owner in enumerate((left, right)):
            got(ag_ref(i, owner), rG.at[i, m])
            ag_send(i, m + 2)

    def q_send(i, k):
        yy = lax.rem(y + k, 4)
        remote(qs.at[i, yy], recvQ.at[i, y], sQ, rQ.at[i], at_t(2 * yy + core)).start()

    def hid(u, i):
        return H[u, i].reshape(128, -1)

    def rows(i):
        got(H.at[1:3, i, 0:2], rG.at[i, 2])
        rg = nn(hid(1, i), wgT[...]) + nn(hid(2, i), wuT[...])
        for q in range(8):
            rgp[i, q % 2, q // 2] = rg[:, 128 * q : 128 * q + 128].astype(BF)
        remote(rgp.at[i, 1 - core], recvP.at[i], sP, rP.at[i], at_t(mate)).start()

    def pair(i):
        got(recvP.at[i], rP.at[i])
        qs[i] = (rgp[i, core].astype(F32) + recvP[i].astype(F32)).astype(BF)
        for k in (2, 1, 3):
            q_send(i, k)

    def back(i):
        tot = qs[i, y].astype(F32)
        got(recvQ.at[i, 0:3], rQ.at[i])
        for k in range(1, 4):
            tot = tot + recvQ[i, lax.rem(y + k, 4)].astype(F32)
        @pl.when(i != 2)
        def _():
            zs[i] = tot.reshape(8, 16, 128).astype(BF)
            x = lax.rem(x0 + i - lax.div(i, 3) + 1, 4)
            for dz in FAR:
                z = lax.rem(z0 + dz, 8)
                pd, pe = lax.div(z, 2), 4 * lax.rem(z, 2) + x
                if dz:
                    remote(zs.at[i, z], recvZ.at[b], sZ, rZ, (pd, pe, t)).start()
                else:
                    @pl.when(i != 4)
                    def _():
                        remote(zs.at[i, z], recvZ.at[b], sZ, rZ, (pd, pe, t)).start()

                    @pl.when(i == 4)
                    def _():
                        pltpu.make_async_copy(zs.at[i, z], recvZ.at[b], rZ).start()

        @pl.when(i == 2)
        def _():
            zr[...] = tot.reshape(16, 8, 128).astype(BF)

            def put(k):
                p = far_first(k)
                remote(zr.at[lax.div(p, 2)], recvZr.at[b], sZr, rZr, at_p(p)).start()

            loop(31, put)
            pltpu.make_async_copy(zr.at[lax.div(b, 2)], recvZr.at[b], rZr).start()

    def turn(i):
        for q in range(8):
            v = XG[q, 0, pl.ds(8 * i, 8)].reshape(128, 128)
            XT[128 * q : 128 * q + 128, pl.ds(pl.multiple_of(128 * i, 128), 128)] = v.T

    def model_grad(u, out):
        out[0] = nn(XT[...], H[u].reshape(640, -1)).astype(BF)

    def down_part(lo, hi):
        g = jnp.concatenate(
            [XG[q, 1, 8 * lo : 8 * hi].reshape(128 * (hi - lo), 128) for q in range(8)], axis=1
        )
        return tn(H[0, lo:hi].reshape(128 * (hi - lo), -1), g)

    loop(S, turn)
    own(0)
    own(1)
    own(2)
    relay(0)
    relay(1)

    def cycle(i):
        @pl.when(i + 3 < S)
        def _():
            own(i + 3)

        @pl.when(i + 2 < S)
        def _():
            relay(i + 2)

        @pl.when(i == S - 3)
        def _():
            for n in range(3):
                for m in (0, 1):
                    hid_send(n, m)

        @pl.when(i >= 1)
        def _():
            pair(i - 1)

        @pl.when(i >= 2)
        def _():
            back(i - 2)

        rows(i)

    loop(S, cycle)
    def hid_relay(n):
        for m, owner in enumerate((left, right)):
            got(hid_ref(n, owner), rN.at[n, m])
            hid_send(n, m + 2)

    pair(S - 1)
    back(S - 2)
    model_grad(1, gg_out)
    back(S - 1)
    hid_relay(0)
    hid_relay(1)
    hid_relay(2)

    got(recvZ, rZ)
    got(recvZr, rZr)
    for dd in range(4):
        at = slice(8 * dd, 8 * dd + 8)
        past16 = recvZr[at].astype(F32).reshape(64, 128).astype(BF)
        z = jnp.concatenate([past16, recvZ[at].reshape(128, 128)], axis=0)
        part_rows = nn(tab[...], z).reshape(8, 8, 128).astype(BF)
        sendY[:, :, 128 * dd : 128 * dd + 128] = part_rows

    def y_send(k):
        q = lax.rem(t + k, 8)
        remote(sendY.at[q], recvY.at[t], sY, rY, at_t(q)).start()

    for k in (4, 3, 5, 2, 6, 1, 7):
        y_send(k)
    recvY[t] = sendY[t]
    model_grad(2, gu_out)
    for n in (0, 1):
        got(H.at[0, HID[n], 0:2], rN.at[n, 2])
    accd[...] = down_part(0, 4)
    g_last[...] = rows_of(1, 4)

    for ref, sem in (
        (recvA.at[:, 0:7], sA), (recvR.at[0:31], sL), (sendC.at[:, 0:31], sC), (XG.at[0:7], sD),
        (rs1, sR1), (raw, sRaw), (red, sRed), (H.at[1:3, :, 0:6], sG), (recvP, sP),
        (recvQ.at[:, 0:3], sQ), (recvZ.at[0:31], sZ), (recvZr.at[0:31], sZr),
    ):
        sent(ref, sem)
    got(recvY.at[0:7], rY)
    for dd in range(4):
        for q in range(8):
            at = slice(1024 * dd + 128 * q, 1024 * dd + 128 * q + 128)
            y_out[:, at] = recvY[q, :, 128 * dd : 128 * dd + 128]
    got(H.at[0, HID[2], 0:2], rN.at[2, 2])
    h_last[...] = H[0, 4].reshape(128, -1)
    sent(recvY.at[0:7], sY)
    sent(H.at[0, :, 0:6], sN)


def put_out(yv, gg, gu, accd, h_last, g_last, y_out, gg_out, gu_out, gd_out, gd, sems):
    copies = [
        pltpu.make_async_copy(src, dst, sems.at[n])
        for n, (src, dst) in enumerate(((gg, gg_out), (gu, gu_out), (yv, y_out), (gd, gd_out)))
    ]
    for c in copies[:3]:
        c.start()
    gd[0] = (accd[...] + tn(h_last[...], g_last[...])).astype(BF)
    copies[3].start()
    for c in copies:
        c.wait()


def shards(tokens, out_grad, route_probs, expert_ids, slot_index, w_gate, w_up, w_down):
    wg, wu, wd = w_gate[0], w_up[0], w_down[0]
    dl, fl = wg.shape
    vm = pl.BlockSpec(memory_space=pltpu.VMEM)
    hbm = pl.BlockSpec(memory_space=pl.ANY)
    dma = pltpu.SemaphoreType.DMA

    def buf(*shape, dtype=BF):
        return pltpu.VMEM(shape, dtype)

    parts = pl.pallas_call(
        kernel,
        name="expert_back",
        out_shape=(
            jax.ShapeDtypeStruct(tokens.shape, BF),
            jax.ShapeDtypeStruct(w_gate.shape, BF),
            jax.ShapeDtypeStruct(w_up.shape, BF),
            jax.ShapeDtypeStruct((fl, dl), F32),
            jax.ShapeDtypeStruct((128, fl), BF),
            jax.ShapeDtypeStruct((128, dl), BF),
        ),
        in_specs=[hbm] * 8,
        out_specs=(vm,) * 6,
        scratch_shapes=[
            buf(8, 4096), buf(8, 4096), buf(2, 64, dtype=F32),
            buf(2, 64, dtype=jnp.int32), buf(2, 64, dtype=jnp.int32),
            buf(dl, fl), buf(dl, fl), buf(fl, dl), buf(fl, dl), buf(fl, dl), buf(dl, fl), buf(64, PLACES),
            buf(2, 8, 8, 512), buf(2, 8, 8, 512),
            buf(32, 8, 128), buf(32, 8, 128), buf(2, 32, 16, 128),
            buf(8, 2, 40, 16, 128), buf(dl, 640), buf(3, 40, 16, fl),
            buf(2, S, 3, 16, fl), buf(2, S, 3, 16, fl), buf(2, S, 3, 16, fl), buf(2, S, 3, 16, fl),
            buf(3, S, 8, 16, fl),
            buf(S, 2, 4, 128, 128), buf(S, 4, 128, 128), buf(S, 4, 128, 128), buf(S, 4, 128, 128),
            buf(S, 8, 16, 128), buf(16, 8, 128), buf(32, 16, 128), buf(32, 8, 128), buf(8, 8, 512), buf(8, 8, 512),
            dma((5,)), dma((3,)), dma((18,)), dma((2,)), dma((S, 2)), dma((S, 2, 2)),
            dma((S, 3)), dma((S, 3)), dma((3, 3)), dma((S,)), dma((S,)),
        ],
        compiler_params=pltpu.CompilerParams(
            collective_id=0, has_side_effects=True, vmem_limit_bytes=46 * 1024 * 1024
        ),
    )(*(
        pltpu.with_memory_space_constraint(v, pltpu.HBM)
        for v in (tokens, out_grad, route_probs.T, expert_ids.T, slot_index.T, wg, wu, wd)
    ))
    return pl.pallas_call(
        put_out,
        name="put_out",
        out_shape=tuple(
            jax.ShapeDtypeStruct(v.shape, BF) for v in (tokens, w_gate, w_up, w_down)
        ),
        in_specs=[vm] * 6,
        out_specs=(hbm,) * 4,
        scratch_shapes=[buf(*w_down.shape), dma((4,))],
        compiler_params=pltpu.CompilerParams(vmem_limit_bytes=16 * 1024 * 1024),
    )(*parts)


def solution(mesh):
    placed = (
        P(("dp", "expert", "tensor"), None),
        P(("dp", "expert", "tensor"), None),
        P(("dp", "expert"), None),
        P(("dp", "expert"), None),
        P(("dp", "expert"), None),
        P("expert", "dp", "tensor"),
        P("expert", "dp", "tensor"),
        P("expert", "tensor", "dp"),
    )
    return jax.shard_map(
        shards,
        mesh=mesh,
        in_specs=placed,
        out_specs=(
            P(("dp", "expert", "tensor"), None),
            P("expert", "dp", "tensor"),
            P("expert", "dp", "tensor"),
            P("expert", "tensor", "dp"),
        ),
        check_vma=False,
    )
```
